256 devices in a mesh: row: 32 (over z, x_hi, core), col: 8 (over y, x_lo).
Axes of the slice: x: 4 (x_hi: 2, x_lo: 2; x = x_hi * 2 + x_lo), y: 4, z: 8, core: 2. Of those that a mesh axis runs over, the one named last changes fastest.
Arguments:
- queries: bfloat16 [262144, 256], P(('row', 'col')), may hold values from -6 to 6
- documents: bfloat16 [8192, 256], P(('row', 'col')), may hold values from -6 to 6
- log_norms: float32 [262144], P(('row', 'col')), may hold values from 7 to 11
- weights: float32 [262144], P(('row', 'col')), may hold values from 1 to 10
- positives: int32 [262144], P(('row', 'col')), may hold values from 0 to 8191
Outputs:
- grad_queries: bfloat16 [262144, 256], P(('row', 'col'))
- grad_documents: bfloat16 [8192, 256], P(('row', 'col'))
- loss: float32 [], replicated
The draws below stay inside these ranges and needn't reach their ends.
All inputs are finite; a program needn't handle non-finite values.
Results may differ from the reference program's by a relative error of at most 0.001.
The reference program's roundings to bfloat16 on the way (of `coeffs`) count: a program that leaves them out, or rounds other values in their place, can miss the bound.
Values may be sent and summed in bfloat16 or wider, within the bound.
No kernel may reach another device: no remote copies, remote signals or barrier semaphores. Data moves between devices by JAX's collectives and lax.ppermute only.
A program may use at most 128 MiB of HBM per device.

```python
import math
import jax
import jax.numpy as jnp
from jax import lax

E = 256
NQ = 262144
ND = 8192


def set_ends(drawn, own_key, smallest, largest):
    dims = drawn.shape
    spot = [jax.random.randint(jax.random.fold_in(own_key, axis), (), 0, dims[axis]) for axis in range(len(dims))]
    drawn = drawn.at[tuple(spot)].set(smallest)
    longest = dims.index(max(dims))
    spot[longest] = (spot[longest] + 1) % dims[longest]
    return drawn.at[tuple(spot)].set(largest)


def levels(rng, extent, split, least, largest):
    def one(axis_at, parts):
        draws = jax.random.uniform(jax.random.fold_in(jax.random.fold_in(rng, 6), axis_at), (parts,), jnp.float32, least / len(split), largest / len(split))
        return jnp.repeat(jnp.exp(draws), extent[axis_at] // parts).reshape((-1,) + (1,) * (len(extent) - axis_at - 1))

    loudness = one(*split[0])
    for cut in split[1:]:
        loudness = loudness * one(*cut)
    return loudness


def noise(key, extent, deviation, most, pieces=(), kind=jnp.bfloat16):
    entries = deviation * jax.random.normal(key, extent, jnp.float32)
    if pieces:
        entries = entries * levels(key, extent, pieces, -0.22, 0.18)
    return jnp.clip(entries, -most, most).astype(kind)


def setup_inputs(seed: int = 0) -> dict:
    arg_keys = jax.random.split(jax.random.key(seed), 6)
    return {
        "queries": noise(arg_keys[0], (NQ, E), 1.0, 6.0, ((0, 256),)),
        "documents": noise(arg_keys[1], (ND, E), 1.0, 6.0, ((0, 256),)),
        "log_norms": jnp.clip(7.0 + 4.0 * jax.random.uniform(arg_keys[2], (NQ,), jnp.float32) ** levels(arg_keys[2], (NQ,), ((0, 256),), -0.2, 0.2), 7.0, 11.0),
        "weights": jnp.clip(jnp.exp(math.log(10.0) - 2.3025851 * jax.random.uniform(arg_keys[3], (NQ,), jnp.float32) ** levels(arg_keys[3], (NQ,), ((0, 256),), -0.2, 0.2)), 1.0, 10.0),
        "positives": set_ends(jax.random.randint(arg_keys[4], (NQ,), 0, ND), jax.random.fold_in(arg_keys[4], 1), 0, ND - 1).astype(jnp.int32),
    }


def reference(queries, documents, log_norms, weights, positives):
    num_q = queries.shape[0]
    num_d = documents.shape[0]
    width = queries.shape[1]
    qblock = math.gcd(num_q, 1024)
    nblocks = num_q // qblock
    doc_ids = jnp.arange(num_d, dtype=jnp.int32)

    def visit(acc, items):
        qrows, lse, wts, pos = items
        scores = jnp.dot(qrows, documents.T, preferred_element_type=jnp.float32) * 0.0625
        probs = jnp.exp(scores - lse[:, None])
        hits = (pos[:, None] == doc_ids[None, :]).astype(jnp.float32)
        pos_scores = jnp.sum(hits * scores, axis=1)
        coeffs = ((probs - hits) * wts[:, None]).astype(jnp.bfloat16)
        grad_q = jnp.dot(coeffs, documents, preferred_element_type=jnp.float32) * 0.0625
        acc = acc + lax.dot_general(coeffs, qrows, (((0,), (0,)), ((), ())), preferred_element_type=jnp.float32)
        part = jnp.sum(wts * (lse - pos_scores))
        return acc, (grad_q.astype(jnp.bfloat16), part)

    items = (queries.reshape(nblocks, qblock, width), log_norms.reshape(nblocks, qblock),
             weights.reshape(nblocks, qblock), positives.reshape(nblocks, qblock))
    acc, outs = lax.scan(visit, jnp.zeros((num_d, width), jnp.float32), items)
    grad_queries = outs[0].reshape(num_q, width)
    grad_documents = (acc * 0.0625).astype(jnp.bfloat16)
    loss = jnp.sum(outs[1]) / num_q
    return grad_queries, grad_documents, loss
```

```python
import functools
import math

import jax
import jax.numpy as jnp
from jax import lax
from jax.experimental import pallas as pl
from jax.experimental.pallas import tpu as pltpu
from jax.sharding import Mesh
from jax.sharding import PartitionSpec as P

AXES = ("z", "xh", "core", "y", "xl")
PLANE = ("xh", "y", "xl")
F32 = jnp.float32
BF16 = jnp.bfloat16
LOG2E = math.log2(math.e)
QT = 256
SUB = 256


def shifted(array, axis):
    return lax.ppermute(array, axis, [(0, 1), (1, 0)])


def to_all(array, axes):
    peers = lax.axis_size(axes)
    return lax.all_to_all(jnp.broadcast_to(array[None], (peers, *array.shape)), axes, 0, 0, tiled=True)


def exchanged(blocks, axes):
    return lax.all_to_all(blocks, axes, 0, 0, tiled=True)


def kernel(nq, nd, docs_ref, ids_ref, q_ref, qt_ref, off_ref, w_ref, pos_ref, gd_ref, gq_ref, ps_ref, dt_ref, c_ref):
    dt_ref[...] = docs_ref[...].T

    @pl.when(pl.program_id(0) == 0)
    def _():
        gq_ref[...] = jnp.zeros(gq_ref.shape, F32)
        ps_ref[...] = jnp.zeros(ps_ref.shape, F32)

    def front(tile, slot):
        cols = pl.ds(pl.multiple_of(tile * QT, QT), QT)
        q_t = qt_ref[:, cols]
        off = off_ref[:, cols]
        w = w_ref[:, cols]
        pos = pos_ref[:, cols]
        found = ps_ref[:, cols]
        for r in range(0, nd, SUB):
            rows = slice(r, r + SUB)
            scores = jnp.dot(docs_ref[rows, :], q_t, preferred_element_type=F32)
            probs = jnp.exp2(scores * (0.0625 * LOG2E) - off)
            hits = jnp.concatenate([ids_ref[rows, :]] * (QT // 128), 1) == pos
            c_ref[slot, rows, :] = (probs - jnp.where(hits, w, 0.0)).astype(BF16)
            found = found + jnp.sum(jnp.where(hits, scores, 0.0).reshape(SUB // 8, 8, QT), 0)
        ps_ref[:, cols] = found

    def back(tile, slot, first):
        cols = pl.ds(pl.multiple_of(tile * QT, QT), QT)
        q = q_ref[cols, :]
        for r in range(0, nd, SUB):
            rows = slice(r, r + SUB)
            term = jnp.dot(c_ref[slot, rows, :], q, preferred_element_type=F32)
            if first:
                gd_ref[rows, :] = term
            else:
                gd_ref[rows, :] += term
        gq_ref[:, cols] += jnp.dot(dt_ref[...], c_ref[slot], preferred_element_type=F32)

    tiles = nq // QT
    front(0, 0)
    front(1, 1)
    back(0, 0, True)

    def pair(i, _):
        tile = 2 * i + 1
        front(tile + 1, 0)
        back(tile, 1, False)
        front(tile + 2, 1)
        back(tile + 1, 0, False)
        return 0

    lax.fori_loop(0, (tiles - 2) // 2, pair, 0)
    back(tiles - 1, 1, False)


def fused(docs, ids, q, q_t, off, w, pos, nd):
    nq, width = q.shape
    total = docs.shape[0]
    whole = lambda *shape: pl.BlockSpec(shape, lambda i: (0, 0))
    return pl.pallas_call(
        functools.partial(kernel, nq, nd),
        grid=(total // nd,),
        in_specs=[
            pl.BlockSpec((nd, width), lambda i: (i, 0)),
            pl.BlockSpec((nd, 128), lambda i: (i, 0)),
            whole(nq, width),
            whole(width, nq),
            whole(1, nq),
            whole(1, nq),
            whole(1, nq),
        ],
        out_specs=[pl.BlockSpec((nd, width), lambda i: (i, 0)), whole(width, nq), whole(8, nq)],
        out_shape=(
            jax.ShapeDtypeStruct((total, width), F32),
            jax.ShapeDtypeStruct((width, nq), F32),
            jax.ShapeDtypeStruct((8, nq), F32),
        ),
        scratch_shapes=[pltpu.VMEM((width, nd), BF16), pltpu.VMEM((2, nd, QT), BF16)],
        compiler_params=pltpu.CompilerParams(vmem_limit_bytes=40 << 20),
        cost_estimate=pl.CostEstimate(flops=6 * nq * total * width, bytes_accessed=16 << 20, transcendentals=nq * total),
        name="fused",
    )(docs, ids, q, q_t, off, w, pos)


def on_device(queries, documents, log_norms, weights, positives):
    own, width = queries.shape
    piece = documents.shape[0]
    total_q = own * lax.axis_size(AXES)
    n_z = lax.axis_size("z")
    n_plane = lax.axis_size(PLANE)
    core = lax.axis_index("core")

    rows = jnp.stack([log_norms, weights, positives.astype(F32)])
    q = jnp.concatenate([queries, shifted(queries, "core")])
    rows = jnp.concatenate([rows, shifted(rows, "core")], 1)
    w = rows[1:2]
    off = rows[0:1] * LOG2E - jnp.log2(w)
    pos = rows[2:3].astype(jnp.int32)

    column = to_all(documents, "z").reshape(n_z * piece, width)
    docs = to_all(column, PLANE).reshape(n_plane * n_z * piece, width)
    shape = (2, 4, 2, n_z, piece, 128)
    at = [lax.broadcasted_iota(jnp.int32, shape, d) for d in range(5)]
    ids = (((at[3] * 2 + at[0]) * 2 + core) * 8 + at[1] * 2 + at[2]) * piece + at[4]
    ids = ids.reshape(n_plane * n_z * piece, 128)

    sums, grad_q, found = fused(docs, ids, q, q.T, off, w, pos, 1024)

    lost = jnp.sum(weights * log_norms) - 0.0625 * jnp.sum(w * found)
    lost = jnp.broadcast_to(lost, (8, width))
    lost = lost + shifted(lost, "core")

    part = exchanged(sums.reshape(n_plane, n_z * piece, width), PLANE).sum(0)
    lost = to_all(lost, PLANE).sum(0)
    part = jnp.concatenate([part.reshape(n_z, piece, width), jnp.broadcast_to(lost[None], (n_z, 8, width))], 1)
    part = exchanged(part, "z").sum(0)
    grad_documents = (part[:piece] * 0.0625).astype(BF16)
    loss = part[piece, 0] / total_q

    grad_q = grad_q[:, :own] + shifted(grad_q[:, own:], "core")
    grad_queries = (grad_q.T * 0.0625).astype(BF16)
    return (grad_queries, grad_documents, loss)


def solution(mesh):
    torus = Mesh(mesh.devices.reshape(8, 2, 2, 4, 2), AXES)
    placed = (P(AXES, None), P(AXES, None), P(AXES), P(AXES), P(AXES))
    return jax.shard_map(
        on_device,
        mesh=torus,
        in_specs=placed,
        out_specs=(P(AXES, None), P(AXES, None), P()),
        check_vma=False,
    )
```

```python
import functools
import math

import jax
import jax.numpy as jnp
from jax import lax
from jax.experimental import pallas as pl
from jax.experimental.pallas import tpu as pltpu
from jax.sharding import Mesh
from jax.sharding import PartitionSpec as P

AXES = ("z", "xh", "core", "y", "xl")
X = ("xh", "xl")
Y = ("y",)
F32 = jnp.float32
BF16 = jnp.bfloat16
LOG2E = math.log2(math.e)
QT = 256
SUB = 256
SIDES = (0, 1, -1, 2)


def other_core(array):
    return lax.ppermute(array, "core", [(0, 1), (1, 0)])


def moved(array, axes, distance):
    if distance == 0:
        return array
    peers = lax.axis_size(axes)
    return lax.ppermute(array, axes, [(i, (i + distance) % peers) for i in range(peers)])


def kernel(n_x, n_y, n_z, side, split, place_ref, xd_ref, yd_ref, q_ref, qt_ref, off_ref, w_ref, pos_ref, *rest):
    if side == 0:
        gq_in = None
    else:
        gq_in, rest = rest[0], rest[1:]
    *gd_refs, gq_ref, ps_ref, d_ref, dt_ref, id_ref, c_ref = rest
    half = xd_ref.shape[0]
    nd = 2 * half
    nq = q_ref.shape[0]
    piece = half // (4 * n_z // 2)
    d_ref[:half, :] = xd_ref[...]
    d_ref[half:, :] = yd_ref[...]
    dt_ref[...] = d_ref[...].T
    x, y, core = place_ref[0], place_ref[1], place_ref[2]
    row = lax.broadcasted_iota(jnp.int32, (piece, 128), 0)
    for block in range(nd // piece):
        group, rest_of = divmod(block, half // piece)
        step, z = divmod(rest_of, n_z // 2)
        dx, dy = (side, SIDES[step]) if group == 0 else (SIDES[step], side)
        from_x = (x - dx + n_x) % n_x
        from_y = (y - dy + n_y) % n_y
        base = (((z + group * (n_z // 2)) * 2 + from_x // 2) * 2 + core) * 2 * n_y + from_y * 2 + from_x % 2
        id_ref[block * piece : (block + 1) * piece, :] = row + base * piece

    def front(tile, slot):
        cols = pl.ds(pl.multiple_of(tile * QT, QT), QT)
        q_t = qt_ref[:, cols]
        off = off_ref[:, cols]
        w = w_ref[:, cols]
        pos = pos_ref[:, cols]
        found = jnp.zeros((8, QT), F32)
        for r in range(0, nd, SUB):
            rows = slice(r, r + SUB)
            scores = jnp.dot(d_ref[rows, :], q_t, preferred_element_type=F32)
            probs = jnp.exp2(scores * (0.0625 * LOG2E) - off)
            hits = jnp.concatenate([id_ref[rows, :]] * (QT // 128), 1) == pos
            c_ref[slot, rows, :] = (probs - jnp.where(hits, w, 0.0)).astype(BF16)
            found = found + jnp.sum(jnp.where(hits, scores, 0.0).reshape(SUB // 8, 8, QT), 0)
        ps_ref[:, cols] = found

    def back(tile, slot, first):
        cols = pl.ds(pl.multiple_of(tile * QT, QT), QT)
        q = q_ref[cols, :]
        for r in range(0, nd, SUB):
            ref = gd_refs[r // split]
            rows = slice(r % split, r % split + SUB)
            term = jnp.dot(c_ref[slot, r : r + SUB, :], q, preferred_element_type=F32)
            if first:
                ref[rows, :] = term
            else:
                ref[rows, :] += term
        term = jnp.dot(dt_ref[...], c_ref[slot], preferred_element_type=F32)
        gq_ref[:, cols] = term if gq_in is None else gq_in[:, cols] + term

    tiles = nq // QT
    front(0, 0)
    front(1, 1)
    back(0, 0, True)

    def pair(i, _):
        tile = 2 * i + 1
        front(tile + 1, 0)
        back(tile, 1, False)
        front(tile + 2, 1)
        back(tile + 1, 0, False)
        return 0

    lax.fori_loop(0, (tiles - 2) // 2, pair, 0)
    back(tiles - 1, 1, False)


def fused(side, split, place, x_docs, y_docs, q, q_t, off, w, pos, grad_q, sizes):
    nq, width = q.shape
    nd = 2 * x_docs.shape[0]
    vmem = pl.BlockSpec(memory_space=pltpu.VMEM)
    operands = [place, x_docs, y_docs, q, q_t, off, w, pos]
    aliases = {}
    outs = nd // split
    if grad_q is not None:
        aliases = {len(operands): outs}
        operands.append(grad_q)
    return pl.pallas_call(
        functools.partial(kernel, *sizes, side, split),
        in_specs=[pl.BlockSpec(memory_space=pltpu.SMEM)] + [vmem] * (len(operands) - 1),
        out_specs=[vmem] * (outs + 2),
        out_shape=[jax.ShapeDtypeStruct((split, width), F32)] * outs
        + [jax.ShapeDtypeStruct((width, nq), F32), jax.ShapeDtypeStruct((8, nq), F32)],
        scratch_shapes=[
            pltpu.VMEM((nd, width), BF16),
            pltpu.VMEM((width, nd), BF16),
            pltpu.VMEM((nd, 128), jnp.int32),
            pltpu.VMEM((2, nd, QT), BF16),
        ],
        input_output_aliases=aliases,
        compiler_params=pltpu.CompilerParams(vmem_limit_bytes=24 << 20),
        cost_estimate=pl.CostEstimate(flops=6 * nq * nd * width, bytes_accessed=8 << 20, transcendentals=nq * nd),
        name="fused",
    )(*operands)


def all_sides(array, axes):
    return {side: moved(array, axes, side) for side in (0, 2, 1, -1)}


def on_device(queries, documents, log_norms, weights, positives):
    own, width = queries.shape
    piece = documents.shape[0]
    total_q = own * lax.axis_size(AXES)
    n_x, n_y, n_z = lax.axis_size(X), lax.axis_size(Y), lax.axis_size("z")
    place = jnp.stack([lax.axis_index(X), lax.axis_index(Y), lax.axis_index("core")]).astype(jnp.int32)

    rows = jnp.stack([log_norms, weights, positives.astype(F32)])
    q = jnp.concatenate([queries, other_core(queries)])
    rows = jnp.concatenate([rows, other_core(rows)], 1)
    w = rows[1:2]
    off = rows[0:1] * LOG2E - jnp.log2(w)
    pos = rows[2:3].astype(jnp.int32)
    q_t = q.T

    column = lax.all_to_all(jnp.broadcast_to(documents[None], (n_z, piece, width)), "z", 0, 0, tiled=True)
    x_part, y_part = column.reshape(2, n_z // 2 * piece, width)
    x_near = all_sides(x_part, Y)
    y_near = all_sides(y_part, X)
    x_docs = all_sides(jnp.concatenate([x_near[s] for s in SIDES]), X)
    y_docs = all_sides(jnp.concatenate([y_near[s] for s in SIDES]), Y)

    half = x_docs[0].shape[0]
    grad_q = None
    terms = {}
    found = 0.0
    for side in (0, -1, 2, 1):
        split = half // 2 if side == 2 else half
        *terms[side], grad_q, seen = fused(
            side, split, place, x_docs[side], y_docs[side], q, q_t, off, w, pos, grad_q, (n_x, n_y, n_z)
        )
        found = found + seen

    lost = jnp.sum(weights * log_norms) - 0.0625 * jnp.sum(w * found)
    lost = jnp.broadcast_to(lost, (8, width))
    lost = lost + other_core(lost)
    for axes in (X, Y):
        lost = lost + moved(lost, axes, 2)
        lost = lost + moved(lost, axes, 1)

    def reduced(own_term, ahead, behind, far_a, far_b, axes, across):
        n = half // 2
        ahead = ahead.at[:n].add(moved(far_a, axes, -1))
        behind = behind.at[n:].add(moved(far_b, axes, 1))
        total = own_term + moved(ahead, axes, -1) + moved(behind, axes, 1)
        parts = total.reshape(4, half // 4, width)
        return sum(moved(parts[i], across, -s) for i, s in enumerate(SIDES))

    x_sum = reduced(terms[0][0], terms[1][0], terms[-1][0], terms[2][0], terms[2][1], X, Y)
    y_sum = reduced(terms[0][1], terms[1][1], terms[-1][1], terms[2][2], terms[2][3], Y, X)
    part = jnp.concatenate([x_sum, y_sum]).reshape(n_z, piece, width)
    part = jnp.concatenate([part, jnp.broadcast_to(lost[None], (n_z, 8, width))], 1)
    part = lax.all_to_all(part, "z", 0, 0, tiled=True).sum(0)
    grad_documents = (part[:piece] * 0.0625).astype(BF16)
    loss = part[piece, 0] / total_q

    grad_q = grad_q[:, :own] + other_core(grad_q[:, own:])
    grad_queries = (grad_q.T * 0.0625).astype(BF16)
    return (grad_queries, grad_documents, loss)


def solution(mesh):
    torus = Mesh(mesh.devices.reshape(8, 2, 2, 4, 2), AXES)
    placed = (P(AXES, None), P(AXES, None), P(AXES), P(AXES), P(AXES))
    return jax.shard_map(
        on_device,
        mesh=torus,
        in_specs=placed,
        out_specs=(P(AXES, None), P(AXES, None), P()),
        check_vma=False,
    )
```

```python
import functools
import math

import jax
import jax.numpy as jnp
from jax import lax
from jax.experimental import pallas as pl
from jax.experimental.pallas import tpu as pltpu
from jax.sharding import Mesh
from jax.sharding import PartitionSpec as P


AXES = ("z", "xh", "core", "y", "xl")
X = ("xh", "xl")
Y = ("y",)
F32 = jnp.float32
BF16 = jnp.bfloat16
LOG2E = math.log2(math.e)
QT = 256
SUB = 256
SIDES = (0, 1, -1, 2)
SIDES_IN_TURN = (0, -1, 2, 1)
VMEM_LIMIT = 16 << 20


def other_core(array):
    return lax.ppermute(array, "core", [(0, 1), (1, 0)])


def moved(array, axes, distance):
    if distance == 0:
        return array
    peers = lax.axis_size(axes)
    return lax.ppermute(array, axes, [(i, (i + distance) % peers) for i in range(peers)])


def kernel(sizes, side, split, *refs):
    n_x, n_y, n_z = sizes
    place_ref, xd_ref, yd_ref, off_ref, w_ref, pos_ref, *refs = refs
    nq = off_ref.shape[1]
    if side == SIDES_IN_TURN[0]:
        own_ref, other_ref, *refs = refs
    else:
        q_ref, qt_ref, gq_in, found_in, *refs = refs
    half = xd_ref.shape[0]
    nd = 2 * half
    outs = nd // split
    gd_refs, refs = refs[:outs], refs[outs:]
    gq_ref, found_ref, *refs = refs
    if side == SIDES_IN_TURN[0]:
        q_ref, qt_ref, *refs = refs
    dt_ref, id_ref, c_ref, gd_ref, sems = refs

    if side == SIDES_IN_TURN[0]:
        for i, ref in enumerate((own_ref, other_ref)):
            part = slice(i * (nq // 2), (i + 1) * (nq // 2))
            q_ref[part, :] = ref[...]
            qt_ref[:, part] = ref[...].T
    gd_ref[...] = jnp.zeros(gd_ref.shape, F32)
    piece = half // (4 * n_z // 2)
    x, y, core = place_ref[0], place_ref[1], place_ref[2]
    row = lax.broadcasted_iota(jnp.int32, (piece, 128), 0)
    for block in range(nd // piece):
        group, rest_of = divmod(block, half // piece)
        step, z = divmod(rest_of, n_z // 2)
        dx, dy = (side, SIDES[step]) if group == 0 else (SIDES[step], side)
        from_x = (x - dx + n_x) % n_x
        from_y = (y - dy + n_y) % n_y
        base = (((z + group * (n_z // 2)) * 2 + from_x // 2) * 2 + core) * 2 * n_y + from_y * 2 + from_x % 2
        id_ref[block * piece : (block + 1) * piece, :] = row + base * piece
    for i, ref in enumerate((xd_ref, yd_ref)):
        dt_ref[:, i * half : (i + 1) * half] = ref[...].T

    def front(tile, slot):
        cols = pl.ds(pl.multiple_of(tile * QT, QT), QT)
        q_t = qt_ref[:, cols]
        off = off_ref[:, cols]
        w = w_ref[:, cols]
        pos = pos_ref[:, cols]
        found = jnp.zeros((8, QT), F32)
        for r in range(0, nd, SUB):
            rows = slice(r, r + SUB)
            docs = (xd_ref, yd_ref)[r // half][r % half : r % half + SUB, :]
            scores = jnp.dot(docs, q_t, preferred_element_type=F32)
            probs = jnp.exp2(scores * (0.0625 * LOG2E) - off)
            hits = jnp.concatenate([id_ref[rows, :]] * (QT // 128), 1) == pos
            c_ref[slot, rows, :] = (probs - jnp.where(hits, w, 0.0)).astype(BF16)
            found = found + jnp.sum(jnp.where(hits, scores, 0.0).reshape(SUB // 8, 8, QT), 0)
        found_ref[:, cols] = found if side == SIDES_IN_TURN[0] else found_in[:, cols] + found

    def back(tile, slot):
        cols = pl.ds(pl.multiple_of(tile * QT, QT), QT)
        q = q_ref[cols, :]
        for r in range(0, nd, SUB):
            gd_ref[r : r + SUB, :] += jnp.dot(c_ref[slot, r : r + SUB, :], q, preferred_element_type=F32)
        term = jnp.dot(dt_ref[...], c_ref[slot], preferred_element_type=F32)
        gq_ref[:, cols] = term if side == SIDES_IN_TURN[0] else gq_in[:, cols] + term

    tiles = nq // QT
    front(0, 0)

    def pair(i, _):
        front(2 * i + 1, 1)
        back(2 * i, 0)
        front((2 * i + 2) % tiles, 0)
        back(2 * i + 1, 1)
        return 0

    lax.fori_loop(0, tiles // 2, pair, 0)
    leave = [
        pltpu.make_async_copy(gd_ref.at[pl.ds(i * split, split)], gd_refs[i], sems.at[i]) for i in range(outs)
    ]
    for copy in leave:
        copy.start()
    for copy in leave:
        copy.wait()


def fused(side, split, place, x_docs, y_docs, off, w, pos, extra, sizes):
    nq = off.shape[1]
    width = x_docs.shape[1]
    nd = 2 * x_docs.shape[0]
    vmem = pl.BlockSpec(memory_space=pltpu.VMEM)
    hbm = pl.BlockSpec(memory_space=pltpu.HBM)
    first = side == SIDES_IN_TURN[0]
    operands = [place, x_docs, y_docs, off, w, pos, *extra]
    outs = nd // split
    out_shape = [pltpu.HBM((split, width), F32)] * outs
    out_shape += [jax.ShapeDtypeStruct((width, nq), F32), jax.ShapeDtypeStruct((8, nq), F32)]
    if first:
        out_shape += [jax.ShapeDtypeStruct((nq, width), BF16), jax.ShapeDtypeStruct((width, nq), BF16)]
    return pl.pallas_call(
        functools.partial(kernel, sizes, side, split),
        in_specs=[pl.BlockSpec(memory_space=pltpu.SMEM)] + [vmem] * (len(operands) - 1),
        out_specs=[hbm] * outs + [vmem] * (len(out_shape) - outs),
        out_shape=out_shape,
        scratch_shapes=[
            pltpu.VMEM((width, nd), BF16),
            pltpu.VMEM((nd, 128), jnp.int32),
            pltpu.VMEM((2, nd, QT), BF16),
            pltpu.VMEM((nd, width), F32),
            pltpu.SemaphoreType.DMA((outs,)),
        ],
        input_output_aliases={} if first else {8: outs},
        compiler_params=pltpu.CompilerParams(vmem_limit_bytes=VMEM_LIMIT),
        cost_estimate=pl.CostEstimate(flops=6 * nq * nd * width, bytes_accessed=8 << 20, transcendentals=nq * nd),
        name="fused",
    )(*operands)


def all_sides(array, axes):
    return {side: moved(array, axes, side) for side in (0, 2, 1, -1)}


def on_device(queries, documents, log_norms, weights, positives):
    own, width = queries.shape
    piece = documents.shape[0]
    total_q = own * lax.axis_size(AXES)
    n_x, n_y, n_z = lax.axis_size(X), lax.axis_size(Y), lax.axis_size("z")
    place = jnp.stack([lax.axis_index(X), lax.axis_index(Y), lax.axis_index("core")]).astype(jnp.int32)

    rows = jnp.stack([log_norms, weights, positives.astype(F32)])
    rows = jnp.concatenate([rows, other_core(rows)], 1)
    other_queries = other_core(queries)
    w = rows[1:2]
    off = rows[0:1] * LOG2E - jnp.log2(w)
    pos = rows[2:3].astype(jnp.int32)

    column = lax.all_to_all(jnp.broadcast_to(documents[None], (n_z, piece, width)), "z", 0, 0, tiled=True)
    x_part, y_part = column.reshape(2, n_z // 2 * piece, width)
    x_near = all_sides(x_part, Y)
    y_near = all_sides(y_part, X)
    x_docs = all_sides(jnp.concatenate([x_near[s] for s in SIDES]), X)
    y_docs = all_sides(jnp.concatenate([y_near[s] for s in SIDES]), Y)

    half = x_docs[0].shape[0]
    terms = {}
    extra = (queries, other_queries)
    for side in SIDES_IN_TURN:
        split = half // 2 if side == 2 else half
        outs = 2 * half // split
        got = fused(side, split, place, x_docs[side], y_docs[side], off, w, pos, extra, (n_x, n_y, n_z))
        terms[side] = got[:outs]
        grad_q, found = got[outs : outs + 2]
        layouts = got[outs + 2 :] or layouts
        extra = (*layouts, grad_q, found)

    ends = (weights * log_norms).reshape(-1, width).sum(0)
    lost = -0.0625 * (w * found).reshape(8, -1, width).sum(1)
    lost = lost.at[0].add(ends)
    lost = lost + other_core(lost)

    def ring(own_term, ahead, behind, far_a, far_b, axes):
        n = half // 2
        tail = lost if axes == X else None
        far_a = moved(far_a, axes, -1)
        far_b = moved(far_b, axes, 1)
        ahead = jnp.concatenate([ahead[:n] + far_a, ahead[n:], *([] if tail is None else [tail])])
        behind = jnp.concatenate([behind[:n], behind[n:] + far_b, *([] if tail is None else [tail])])
        ahead, behind = moved(ahead, axes, -1), moved(behind, axes, 1)
        total = own_term + ahead[:half] + behind[:half]
        return (total, None) if tail is None else (total, tail + moved(tail, axes, 2) + ahead[half:] + behind[half:])

    x_total, x_lost = ring(terms[0][0], terms[1][0], terms[-1][0], terms[2][0], terms[2][1], X)
    y_total, _ = ring(terms[0][1], terms[1][1], terms[-1][1], terms[2][2], terms[2][3], Y)
    n = half // 4
    x_sum = sum(
        moved(jnp.concatenate([x_total[i * n : (i + 1) * n], x_lost]), Y, -s) for i, s in enumerate(SIDES)
    )
    y_sum = sum(moved(y_total[i * n : (i + 1) * n], X, -s) for i, s in enumerate(SIDES))
    part = jnp.concatenate([x_sum[:n], y_sum]).reshape(n_z, piece, width)
    part = jnp.concatenate([part, jnp.broadcast_to(x_sum[n:][None], (n_z, 8, width))], 1)
    part = lax.all_to_all(part, "z", 0, 0, tiled=True).sum(0)
    grad_documents = (part[:piece] * 0.0625).astype(BF16)
    loss = jnp.sum(part[piece:]) / total_q

    grad_q = grad_q[:, :own] + other_core(grad_q[:, own:])
    grad_queries = (grad_q.T * 0.0625).astype(BF16)
    return (grad_queries, grad_documents, loss)


def solution(mesh):
    torus = Mesh(mesh.devices.reshape(8, 2, 2, 4, 2), AXES)
    placed = (P(AXES, None), P(AXES, None), P(AXES), P(AXES), P(AXES))
    return jax.shard_map(
        on_device,
        mesh=torus,
        in_specs=placed,
        out_specs=(P(AXES, None), P(AXES, None), P()),
        check_vma=False,
    )
```

```python
import functools
import math

import jax
import jax.numpy as jnp
from jax import lax
from jax.experimental import pallas as pl
from jax.experimental.pallas import tpu as pltpu
from jax.sharding import Mesh
from jax.sharding import PartitionSpec as P


AXES = ("z", "xh", "core", "y", "xl")
X = ("xh", "xl")
Y = ("y",)
F32 = jnp.float32
BF16 = jnp.bfloat16
LOG2E = math.log2(math.e)
QT = 256
SUB = 256
SIDES = (0, 1, -1, 2)
SIDES_IN_TURN = (0, -1, 2, 1)
VMEM_LIMIT = 16 << 20


def other_core(array):
    return lax.ppermute(array, "core", [(0, 1), (1, 0)])


def moved(array, axes, distance):
    if distance == 0:
        return array
    peers = lax.axis_size(axes)
    return lax.ppermute(array, axes, [(i, (i + distance) % peers) for i in range(peers)])


def kernel(sizes, side, split, *refs):
    n_x, n_y, n_z = sizes
    first, last = side == SIDES_IN_TURN[0], side == SIDES_IN_TURN[-1]
    place_ref, xd_ref, yd_ref, off_ref, w_ref, pos_ref, ends_ref, *refs = refs
    nq = off_ref.shape[1]
    if first:
        own_ref, other_ref, *refs = refs
    else:
        q_ref, qt_ref, gq_in, found_in, *refs = refs
    half = xd_ref.shape[0]
    nd = 2 * half
    outs = nd // split
    gd_refs, refs = refs[:outs], refs[outs:]
    gq_ref, found_ref, *refs = refs
    if first:
        q_ref, qt_ref, *refs = refs
    dt_ref, id_ref, c_ref, gd_ref, sems = refs

    if first:
        own = pltpu.make_async_copy(own_ref, q_ref.at[: nq // 2], sems.at[nd // SUB])
        own.start()
        q_ref[nq // 2 :, :] = other_ref[...]
        qt_ref[:, nq // 2 :] = other_ref[...].T
    if last:
        top = lax.broadcasted_iota(jnp.int32, found_ref.shape, 0) == 0
        found_ref[...] = jnp.where(top, ends_ref[...], 0.0)
    piece = half // (4 * n_z // 2)
    x, y, core = place_ref[0], place_ref[1], place_ref[2]
    row = lax.broadcasted_iota(jnp.int32, (piece, 128), 0)
    for block in range(nd // piece):
        group, rest_of = divmod(block, half // piece)
        step, z = divmod(rest_of, n_z // 2)
        dx, dy = (side, SIDES[step]) if group == 0 else (SIDES[step], side)
        from_x = (x - dx + n_x) % n_x
        from_y = (y - dy + n_y) % n_y
        base = (((z + group * (n_z // 2)) * 2 + from_x // 2) * 2 + core) * 2 * n_y + from_y * 2 + from_x % 2
        id_ref[block * piece : (block + 1) * piece, :] = row + base * piece
    for i, ref in enumerate((xd_ref, yd_ref)):
        dt_ref[:, i * half : (i + 1) * half] = ref[...].T
    if first:
        own.wait()
        qt_ref[:, : nq // 2] = q_ref[: nq // 2, :].T

    def front(tile, slot):
        cols = pl.ds(pl.multiple_of(tile * QT, QT), QT)
        q_t = qt_ref[:, cols]
        off = off_ref[:, cols]
        w = w_ref[:, cols]
        pos = pos_ref[:, cols]
        found = jnp.zeros((8, QT), F32)
        for r in range(0, nd, SUB):
            docs = (xd_ref, yd_ref)[r // half][r % half : r % half + SUB, :]
            scores = jnp.dot(docs, q_t, preferred_element_type=F32)
            probs = jnp.exp2(scores * (0.0625 * LOG2E) - off)
            hits = jnp.concatenate([id_ref[r : r + SUB, :]] * (QT // 128), 1) == pos
            c_ref[slot, r : r + SUB, :] = (probs - jnp.where(hits, w, 0.0)).astype(BF16)
            found = found + jnp.sum(jnp.where(hits, scores, 0.0).reshape(SUB // 8, 8, QT), 0)
        if not first:
            found = found_in[:, cols] + found
        if last:
            found_ref[...] -= 0.0625 * w * found
        else:
            found_ref[:, cols] = found

    def back(tile, slot, opening=False, closing=False):
        cols = pl.ds(pl.multiple_of(tile * QT, QT), QT)
        q = q_ref[cols, :]
        leave = []
        for r in range(0, nd, SUB):
            rows = slice(r, r + SUB)
            term = jnp.dot(c_ref[slot, rows, :], q, preferred_element_type=F32)
            gd_ref[rows, :] = term if opening else gd_ref[rows, :] + term
            if closing:
                out = gd_refs[r // split].at[pl.ds(r % split, SUB)]
                leave.append(pltpu.make_async_copy(gd_ref.at[rows], out, sems.at[r // SUB]))
                leave[-1].start()
        term = jnp.dot(dt_ref[...], c_ref[slot], preferred_element_type=F32)
        gq_ref[:, cols] = term if first else gq_in[:, cols] + term
        for copy in leave:
            copy.wait()

    tiles = nq // QT
    front(0, 0)
    front(1, 1)
    back(0, 0, opening=True)

    def pair(i, _):
        tile = 2 * i + 1
        front(tile + 1, 0)
        back(tile, 1)
        front(tile + 2, 1)
        back(tile + 1, 0)
        return 0

    lax.fori_loop(0, (tiles - 2) // 2, pair, 0)
    back(tiles - 1, 1, closing=True)


def fused(side, split, place, x_docs, y_docs, off, w, pos, ends, extra, sizes):
    nq = off.shape[1]
    width = x_docs.shape[1]
    nd = 2 * x_docs.shape[0]
    vmem = pl.BlockSpec(memory_space=pltpu.VMEM)
    hbm = pl.BlockSpec(memory_space=pltpu.HBM)
    first, last = side == SIDES_IN_TURN[0], side == SIDES_IN_TURN[-1]
    operands = [place, x_docs, y_docs, off, w, pos, ends, *extra]
    outs = nd // split
    out_shape = [pltpu.HBM((split, width), F32)] * outs
    out_shape += [jax.ShapeDtypeStruct((width, nq), F32), jax.ShapeDtypeStruct((8, QT if last else nq), F32)]
    if first:
        out_shape += [jax.ShapeDtypeStruct((nq, width), BF16), jax.ShapeDtypeStruct((width, nq), BF16)]
    return pl.pallas_call(
        functools.partial(kernel, sizes, side, split),
        in_specs=[pl.BlockSpec(memory_space=pltpu.SMEM)] + [vmem] * 6 + [hbm if first else vmem] + [vmem] * (len(operands) - 8),
        out_specs=[hbm] * outs + [vmem] * (len(out_shape) - outs),
        out_shape=out_shape,
        scratch_shapes=[
            pltpu.VMEM((width, nd), BF16),
            pltpu.VMEM((nd, 128), jnp.int32),
            pltpu.VMEM((2, nd, QT), BF16),
            pltpu.VMEM((nd, width), F32),
            pltpu.SemaphoreType.DMA((nd // SUB + 1,)),
        ],
        input_output_aliases={} if first else {9: outs},
        compiler_params=pltpu.CompilerParams(vmem_limit_bytes=VMEM_LIMIT),
        cost_estimate=pl.CostEstimate(flops=6 * nq * nd * width, bytes_accessed=8 << 20, transcendentals=nq * nd),
        name="fused",
    )(*operands)


def all_sides(array, axes):
    return {side: moved(array, axes, side) for side in (0, 2, 1, -1)}


def on_device(queries, documents, log_norms, weights, positives):
    own, width = queries.shape
    piece = documents.shape[0]
    total_q = own * lax.axis_size(AXES)
    n_x, n_y, n_z = lax.axis_size(X), lax.axis_size(Y), lax.axis_size("z")
    place = jnp.stack([lax.axis_index(X), lax.axis_index(Y), lax.axis_index("core")]).astype(jnp.int32)

    rows = jnp.stack([log_norms, weights, positives.astype(F32)])
    rows = jnp.concatenate([rows, other_core(rows)], 1)
    other_queries = other_core(queries)
    w = rows[1:2]
    off = rows[0:1] * LOG2E - jnp.log2(w)
    pos = rows[2:3].astype(jnp.int32)

    column = lax.all_to_all(jnp.broadcast_to(documents[None], (n_z, piece, width)), "z", 0, 0, tiled=True)
    x_part, y_part = column.reshape(2, n_z // 2 * piece, width)
    x_near = all_sides(x_part, Y)
    y_near = all_sides(y_part, X)
    x_docs = all_sides(jnp.concatenate([x_near[s] for s in SIDES]), X)
    y_docs = all_sides(jnp.concatenate([y_near[s] for s in SIDES]), Y)

    half = x_docs[0].shape[0]
    terms = {}
    ends = (weights * log_norms).reshape(-1, QT).sum(0)[None]
    extra = (pltpu.with_memory_space_constraint(queries, pltpu.HBM), other_queries)
    for side in SIDES_IN_TURN:
        split = half // 2 if side == 2 else half
        outs = 2 * half // split
        got = fused(side, split, place, x_docs[side], y_docs[side], off, w, pos, ends, extra, (n_x, n_y, n_z))
        terms[side] = got[:outs]
        grad_q, found = got[outs : outs + 2]
        layouts = got[outs + 2 :] or layouts
        extra = (*layouts, grad_q, found)

    lost = found + other_core(found)

    def ring(own_term, ahead, behind, far_a, far_b, axes):
        n = half // 2
        tail = lost if axes == X else None
        far_a = moved(far_a, axes, -1)
        far_b = moved(far_b, axes, 1)
        ahead = jnp.concatenate([ahead[:n] + far_a, ahead[n:], *([] if tail is None else [tail])])
        behind = jnp.concatenate([behind[:n], behind[n:] + far_b, *([] if tail is None else [tail])])
        ahead, behind = moved(ahead, axes, -1), moved(behind, axes, 1)
        total = own_term + ahead[:half] + behind[:half]
        return (total, None) if tail is None else (total, tail + moved(tail, axes, 2) + ahead[half:] + behind[half:])

    x_total, x_lost = ring(terms[0][0], terms[1][0], terms[-1][0], terms[2][0], terms[2][1], X)
    y_total, _ = ring(terms[0][1], terms[1][1], terms[-1][1], terms[2][2], terms[2][3], Y)
    n = half // 4
    x_sum = sum(
        moved(jnp.concatenate([x_total[i * n : (i + 1) * n], x_lost]), Y, -s) for i, s in enumerate(SIDES)
    )
    y_sum = sum(moved(y_total[i * n : (i + 1) * n], X, -s) for i, s in enumerate(SIDES))
    part = jnp.concatenate([x_sum[:n], y_sum]).reshape(n_z, piece, width)
    part = jnp.concatenate([part, jnp.broadcast_to(x_sum[n:][None], (n_z, 8, width))], 1)
    part = lax.all_to_all(part, "z", 0, 0, tiled=True).sum(0)
    grad_documents = (part[:piece] * 0.0625).astype(BF16)
    loss = jnp.sum(part[piece:]) / total_q

    grad_q = grad_q[:, :own] + other_core(grad_q[:, own:])
    grad_queries = (grad_q.T * 0.0625).astype(BF16)
    return (grad_queries, grad_documents, loss)


def solution(mesh):
    torus = Mesh(mesh.devices.reshape(8, 2, 2, 4, 2), AXES)
    placed = (P(AXES, None), P(AXES, None), P(AXES), P(AXES), P(AXES))
    return jax.shard_map(
        on_device,
        mesh=torus,
        in_specs=placed,
        out_specs=(P(AXES, None), P(AXES, None), P()),
        check_vma=False,
    )
```

```python
import functools
import math

import jax
import jax.numpy as jnp
from jax import lax
from jax.experimental import pallas as pl
from jax.experimental.pallas import tpu as pltpu
from jax.sharding import Mesh
from jax.sharding import PartitionSpec as P


AXES = ("z", "xh", "core", "y", "xl")
X = ("xh", "xl")
Y = ("y",)
F32 = jnp.float32
BF16 = jnp.bfloat16
LOG2E = math.log2(math.e)
QT = 256
SUB = 256
SIDES = (0, 1, -1, 2)
SIDES_IN_TURN = (0, -1, 2, 1)
VMEM_LIMIT = 16 << 20


def other_core(array):
    return lax.ppermute(array, "core", [(0, 1), (1, 0)])


def moved(array, axes, distance):
    if distance == 0:
        return array
    peers = lax.axis_size(axes)
    return lax.ppermute(array, axes, [(i, (i + distance) % peers) for i in range(peers)])


def layout_kernel(own_ref, other_ref, rows_ref, other_rows_ref, q_ref, qt_ref, off_ref, w_ref, pos_ref, sem):
    n = own_ref.shape[0]
    own = pltpu.make_async_copy(own_ref, q_ref.at[:n], sem)
    own.start()
    for i, ref in enumerate((rows_ref, other_rows_ref)):
        part = slice(i * n, (i + 1) * n)
        w_ref[:, part] = ref[1:2, :]
        off_ref[:, part] = ref[0:1, :] * LOG2E - jnp.log2(ref[1:2, :])
        pos_ref[:, part] = ref[2:3, :].astype(jnp.int32)
    q_ref[n:, :] = other_ref[...]
    qt_ref[:, n:] = other_ref[...].T
    own.wait()
    qt_ref[:, :n] = q_ref[:n, :].T


def layout(queries, other_queries, rows, other_rows):
    n, width = queries.shape
    vmem = pl.BlockSpec(memory_space=pltpu.VMEM)
    line = jax.ShapeDtypeStruct((1, 2 * n), F32)
    return pl.pallas_call(
        layout_kernel,
        in_specs=[pl.BlockSpec(memory_space=pltpu.HBM)] + [vmem] * 3,
        out_specs=[vmem] * 5,
        out_shape=[
            jax.ShapeDtypeStruct((2 * n, width), BF16),
            jax.ShapeDtypeStruct((width, 2 * n), BF16),
            line,
            line,
            jax.ShapeDtypeStruct((1, 2 * n), jnp.int32),
        ],
        scratch_shapes=[pltpu.SemaphoreType.DMA],
        compiler_params=pltpu.CompilerParams(vmem_limit_bytes=VMEM_LIMIT),
        name="layout",
    )(pltpu.with_memory_space_constraint(queries, pltpu.HBM), other_queries, rows, other_rows)


def kernel(sizes, side, split, *refs):
    n_x, n_y, n_z = sizes
    first, last = side == SIDES_IN_TURN[0], side == SIDES_IN_TURN[-1]
    place_ref, xd_ref, yd_ref, q_ref, qt_ref, off_ref, w_ref, pos_ref, ends_ref, *refs = refs
    nq = off_ref.shape[1]
    if not first:
        gq_in, found_in, *refs = refs
    half = xd_ref.shape[0]
    nd = 2 * half
    outs = nd // split
    gd_refs, refs = refs[:outs], refs[outs:]
    gq_ref, found_ref, *refs = refs
    dt_ref, id_ref, c_ref, gd_ref, sems = refs

    if last:
        top = lax.broadcasted_iota(jnp.int32, found_ref.shape, 0) == 0
        found_ref[...] = jnp.where(top, ends_ref[...], 0.0)
    piece = half // (4 * n_z // 2)
    x, y, core = place_ref[0], place_ref[1], place_ref[2]
    row = lax.broadcasted_iota(jnp.int32, (piece, 128), 0)
    for block in range(nd // piece):
        group, rest_of = divmod(block, half // piece)
        step, z = divmod(rest_of, n_z // 2)
        dx, dy = (side, SIDES[step]) if group == 0 else (SIDES[step], side)
        from_x = (x - dx + n_x) % n_x
        from_y = (y - dy + n_y) % n_y
        base = (((z + group * (n_z // 2)) * 2 + from_x // 2) * 2 + core) * 2 * n_y + from_y * 2 + from_x % 2
        id_ref[block * piece : (block + 1) * piece, :] = row + base * piece
    for i, ref in enumerate((xd_ref, yd_ref)):
        dt_ref[:, i * half : (i + 1) * half] = ref[...].T

    def front(tile, slot):
        cols = pl.ds(pl.multiple_of(tile * QT, QT), QT)
        q_t = qt_ref[:, cols]
        off = off_ref[:, cols]
        w = w_ref[:, cols]
        pos = pos_ref[:, cols]
        found = jnp.zeros((8, QT), F32)
        for r in range(0, nd, SUB):
            docs = (xd_ref, yd_ref)[r // half][r % half : r % half + SUB, :]
            scores = jnp.dot(docs, q_t, preferred_element_type=F32)
            probs = jnp.exp2(scores * (0.0625 * LOG2E) - off)
            hits = jnp.concatenate([id_ref[r : r + SUB, :]] * (QT // 128), 1) == pos
            c_ref[slot, r : r + SUB, :] = (probs - jnp.where(hits, w, 0.0)).astype(BF16)
            found = found + jnp.sum(jnp.where(hits, scores, 0.0).reshape(SUB // 8, 8, QT), 0)
        if not first:
            found = found_in[:, cols] + found
        if last:
            found_ref[...] -= 0.0625 * w * found
        else:
            found_ref[:, cols] = found

    def back(tile, slot, opening=False, closing=False):
        cols = pl.ds(pl.multiple_of(tile * QT, QT), QT)
        q = q_ref[cols, :]
        leave = []
        for r in range(0, nd, SUB):
            rows = slice(r, r + SUB)
            term = jnp.dot(c_ref[slot, rows, :], q, preferred_element_type=F32)
            gd_ref[rows, :] = term if opening else gd_ref[rows, :] + term
            if closing:
                out = gd_refs[r // split].at[pl.ds(r % split, SUB)]
                leave.append(pltpu.make_async_copy(gd_ref.at[rows], out, sems.at[r // SUB]))
                leave[-1].start()
        term = jnp.dot(dt_ref[...], c_ref[slot], preferred_element_type=F32)
        gq_ref[:, cols] = term if first else gq_in[:, cols] + term
        for copy in leave:
            copy.wait()

    tiles = nq // QT
    front(0, 0)
    front(1, 1)
    back(0, 0, opening=True)

    def pair(i, _):
        tile = 2 * i + 1
        front(tile + 1, 0)
        back(tile, 1)
        front(tile + 2, 1)
        back(tile + 1, 0)
        return 0

    lax.fori_loop(0, (tiles - 2) // 2, pair, 0)
    back(tiles - 1, 1, closing=True)


def fused(side, split, place, x_docs, y_docs, asked, ends, sums, sizes):
    nq = asked[0].shape[0]
    width = x_docs.shape[1]
    nd = 2 * x_docs.shape[0]
    vmem = pl.BlockSpec(memory_space=pltpu.VMEM)
    hbm = pl.BlockSpec(memory_space=pltpu.HBM)
    first, last = side == SIDES_IN_TURN[0], side == SIDES_IN_TURN[-1]
    operands = [place, x_docs, y_docs, *asked, ends, *sums]
    outs = nd // split
    out_shape = [pltpu.HBM((split, width), F32)] * outs
    out_shape += [jax.ShapeDtypeStruct((width, nq), F32), jax.ShapeDtypeStruct((8, QT if last else nq), F32)]
    return pl.pallas_call(
        functools.partial(kernel, sizes, side, split),
        in_specs=[pl.BlockSpec(memory_space=pltpu.SMEM)] + [vmem] * (len(operands) - 1),
        out_specs=[hbm] * outs + [vmem] * (len(out_shape) - outs),
        out_shape=out_shape,
        scratch_shapes=[
            pltpu.VMEM((width, nd), BF16),
            pltpu.VMEM((nd, 128), jnp.int32),
            pltpu.VMEM((2, nd, QT), BF16),
            pltpu.VMEM((nd, width), F32),
            pltpu.SemaphoreType.DMA((nd // SUB,)),
        ],
        input_output_aliases={} if first else {9: outs},
        compiler_params=pltpu.CompilerParams(vmem_limit_bytes=VMEM_LIMIT),
        cost_estimate=pl.CostEstimate(flops=6 * nq * nd * width, bytes_accessed=8 << 20, transcendentals=nq * nd),
        name="fused",
    )(*operands)


def all_sides(array, axes):
    return {side: moved(array, axes, side) for side in (0, 2, 1, -1)}


def on_device(queries, documents, log_norms, weights, positives):
    own, width = queries.shape
    piece = documents.shape[0]
    total_q = own * lax.axis_size(AXES)
    n_x, n_y, n_z = lax.axis_size(X), lax.axis_size(Y), lax.axis_size("z")
    place = jnp.stack([lax.axis_index(X), lax.axis_index(Y), lax.axis_index("core")]).astype(jnp.int32)

    rows = jnp.stack([log_norms, weights, positives.astype(F32)])
    asked = layout(queries, other_core(queries), rows, other_core(rows))

    column = lax.all_to_all(jnp.broadcast_to(documents[None], (n_z, piece, width)), "z", 0, 0, tiled=True)
    x_part, y_part = column.reshape(2, n_z // 2 * piece, width)
    x_near = all_sides(x_part, Y)
    y_near = all_sides(y_part, X)
    x_docs = all_sides(jnp.concatenate([x_near[s] for s in SIDES]), X)
    y_docs = all_sides(jnp.concatenate([y_near[s] for s in SIDES]), Y)

    half = x_docs[0].shape[0]
    terms = {}
    ends = (weights * log_norms).reshape(-1, QT).sum(0)[None]
    sums = ()
    for side in SIDES_IN_TURN:
        split = half // 2 if side == 2 else half
        outs = 2 * half // split
        got = fused(side, split, place, x_docs[side], y_docs[side], asked, ends, sums, (n_x, n_y, n_z))
        terms[side] = got[:outs]
        sums = grad_q, lost = got[outs:]

    def ring(own_term, ahead, behind, far_a, far_b, axes):
        n = half // 2
        tail = lost if axes == X else None
        far_a = moved(far_a, axes, -1)
        far_b = moved(far_b, axes, 1)
        ahead = jnp.concatenate([ahead[:n] + far_a, ahead[n:], *([] if tail is None else [tail])])
        behind = jnp.concatenate([behind[:n], behind[n:] + far_b, *([] if tail is None else [tail])])
        ahead, behind = moved(ahead, axes, -1), moved(behind, axes, 1)
        total = own_term + ahead[:half] + behind[:half]
        return (total, None) if tail is None else (total, tail + moved(tail, axes, 2) + ahead[half:] + behind[half:])

    x_total, x_lost = ring(terms[0][0], terms[1][0], terms[-1][0], terms[2][0], terms[2][1], X)
    y_total, _ = ring(terms[0][1], terms[1][1], terms[-1][1], terms[2][2], terms[2][3], Y)
    n = half // 4
    x_sum = sum(
        moved(jnp.concatenate([x_total[i * n : (i + 1) * n], x_lost]), Y, -s) for i, s in enumerate(SIDES)
    )
    y_sum = sum(moved(y_total[i * n : (i + 1) * n], X, -s) for i, s in enumerate(SIDES))
    part = jnp.concatenate([x_sum[:n], y_sum]).reshape(n_z, piece, width)
    part = jnp.concatenate([part, jnp.broadcast_to(x_sum[n:][None], (n_z, 8, width))], 1)
    part = lax.all_to_all(part, "z", 0, 0, tiled=True)
    part = part.sum(0)
    grad_documents = (part[:piece] * 0.0625).astype(BF16)
    lost = jnp.broadcast_to(jnp.sum(part[piece:]), (8, 128))
    loss = (lost + other_core(lost))[0, 0] / total_q

    other_grad = grad_q[:, own:]
    other_grad = other_core(other_grad)
    grad_queries = ((grad_q[:, :own] + other_grad).T * 0.0625).astype(BF16)
    return (grad_queries, grad_documents, loss)


def solution(mesh):
    torus = Mesh(mesh.devices.reshape(8, 2, 2, 4, 2), AXES)
    placed = (P(AXES, None), P(AXES, None), P(AXES), P(AXES), P(AXES))
    return jax.shard_map(
        on_device,
        mesh=torus,
        in_specs=placed,
        out_specs=(P(AXES, None), P(AXES, None), P()),
        check_vma=False,
    )
```

```python
import functools
import itertools
import math

import jax
import jax.numpy as jnp
from jax import lax
from jax.experimental import pallas as pl
from jax.experimental.pallas import tpu as pltpu
from jax.sharding import Mesh
from jax.sharding import PartitionSpec as P


AXES = ("z", "xh", "core", "y", "xl")
X = ("xh", "xl")
Y = ("y",)
CHIPS = ("xh", "core", "y", "xl")
F32 = jnp.float32
BF16 = jnp.bfloat16
LOG2E = math.log2(math.e)
QT = 512
SUB = 256
SIDES = (0, 1, -1, 2)
TURNS = ((0, 0, 4), (2, 0, 4), (-1, 0, 4), (1, 0, 2), (1, 2, 4))
VMEM_LIMIT = 16 << 20


def other_core(array):
    return lax.ppermute(array, "core", [(0, 1), (1, 0)])


def moved(array, along, distance):
    if distance == 0:
        return array
    n_xh, n_y, n_xl = (lax.axis_size(axis) for axis in ("xh", "y", "xl"))
    n_x = n_xh * n_xl

    def at(x, core, y):
        return ((x // n_xl * 2 + core) * n_y + y) * n_xl + x % n_xl

    route = []
    for x, core, y in itertools.product(range(n_x), range(2), range(n_y)):
        in_x = along == (core == 0)
        to = ((x + distance) % n_x, y) if in_x else (x, (y + distance) % n_y)
        route.append((at(x, core, y), at(to[0], core, to[1])))
    return lax.ppermute(array, CHIPS, route)


def lay_out(own_ref, other_ref, rows_ref, other_rows_ref, q_ref, qt_ref, off_ref, w_ref, pos_ref, sem):
    n = own_ref.shape[0]
    own = pltpu.make_async_copy(own_ref, q_ref.at[:n], sem)
    own.start()
    for i, ref in enumerate((rows_ref, other_rows_ref)):
        part = slice(i * n, (i + 1) * n)
        w_ref[:, part] = ref[1:2, :]
        off_ref[:, part] = ref[0:1, :] * LOG2E - jnp.log2(ref[1:2, :])
        pos_ref[:, part] = ref[2:3, :].astype(jnp.int32)
    q_ref[n:, :] = other_ref[...]
    qt_ref[:, n:] = other_ref[...].T
    own.wait()
    qt_ref[:, :n] = q_ref[:n, :].T


def kernel(sizes, turn, split, *refs):
    n_x, n_y, n_z = sizes
    first, last = turn == 0, turn == len(TURNS) - 1
    side, begin, end = TURNS[turn]
    place_ref, d_ref, *refs = refs
    if first:
        given, ends_ref, refs = refs[:4], refs[4], refs[5:]
    else:
        q_ref, qt_ref, off_ref, w_ref, pos_ref, ends_ref, gq_in, found_in, *refs = refs
    piece = d_ref.shape[0] // (len(SIDES) * n_z)
    nd = (end - begin) * n_z * piece
    d_ref = d_ref.at[pl.ds(begin * n_z * piece, nd)]
    outs = nd // split
    gd_refs, refs = refs[:outs], refs[outs:]
    gq_ref, found_ref, *refs = refs
    if first:
        q_ref, qt_ref, off_ref, w_ref, pos_ref, *refs = refs
        lay_out(*given, q_ref, qt_ref, off_ref, w_ref, pos_ref, refs[-1].at[nd // SUB])
    nq = q_ref.shape[0]
    dt_ref, id_ref, c_ref, gd_ref, sems = refs

    if last:
        top = lax.broadcasted_iota(jnp.int32, found_ref.shape, 0) == 0
        found_ref[...] = jnp.where(top, ends_ref[...], 0.0)
    x, y, core = place_ref[0], place_ref[1], place_ref[2]
    row = lax.broadcasted_iota(jnp.int32, (piece, 128), 0)
    for step, across in enumerate(SIDES[begin:end]):
        from_x = (x - jnp.where(core == 0, side, across) + n_x) % n_x
        from_y = (y - jnp.where(core == 0, across, side) + n_y) % n_y
        for j in range(n_z):
            z = j % (n_z // 2) + core * (n_z // 2)
            owner = core if j < n_z // 2 else 1 - core
            base = ((z * 2 + from_x // 2) * 2 + owner) * 2 * n_y + from_y * 2 + from_x % 2
            at = (step * n_z + j) * piece
            id_ref[at : at + piece, :] = row + base * piece
    dt_ref[...] = d_ref[...].T

    def front(tile, slot):
        cols = pl.ds(pl.multiple_of(tile * QT, QT), QT)
        q_t = qt_ref[:, cols]
        off = off_ref[:, cols]
        w = w_ref[:, cols]
        pos = pos_ref[:, cols]
        found = jnp.zeros((8, QT), F32)
        for r in range(0, nd, SUB):
            scores = jnp.dot(d_ref[r : r + SUB, :], q_t, preferred_element_type=F32)
            probs = jnp.exp2(scores * (0.0625 * LOG2E) - off)
            hits = jnp.concatenate([id_ref[r : r + SUB, :]] * (QT // 128), 1) == pos
            c_ref[slot, r : r + SUB, :] = (probs - jnp.where(hits, w, 0.0)).astype(BF16)
            found = found + jnp.sum(jnp.where(hits, scores, 0.0).reshape(SUB // 8, 8, QT), 0)
        if not first:
            found = found_in[:, cols] + found
        if last:
            found = 0.0625 * w * found
            width = found_ref.shape[1]
            for c in range(0, QT, width):
                found_ref[...] -= found[:, c : c + width]
        else:
            found_ref[:, cols] = found

    def back(tile, slot, opening=False, closing=False):
        cols = pl.ds(pl.multiple_of(tile * QT, QT), QT)
        q = q_ref[cols, :]
        leave = []
        for r in range(0, nd, SUB):
            rows = slice(r, r + SUB)
            term = jnp.dot(c_ref[slot, rows, :], q, preferred_element_type=F32)
            gd_ref[rows, :] = term if opening else gd_ref[rows, :] + term
            if closing:
                out = gd_refs[r // split].at[pl.ds(r % split, SUB)]
                leave.append(pltpu.make_async_copy(gd_ref.at[rows], out, sems.at[r // SUB]))
                leave[-1].start()
        term = jnp.dot(dt_ref[...], c_ref[slot], preferred_element_type=F32)
        gq_ref[:, cols] = term if first else gq_in[:, cols] + term
        for copy in leave:
            copy.wait()

    tiles = nq // QT
    front(0, 0)
    front(1, 1)
    back(0, 0, opening=True)

    def pair(i, _):
        tile = 2 * i + 1
        front(tile + 1, 0)
        back(tile, 1)
        front(tile + 2, 1)
        back(tile + 1, 0)
        return 0

    lax.fori_loop(0, (tiles - 2) // 2, pair, 0)
    back(tiles - 1, 1, closing=True)


def fused(turn, split, place, docs, asked, ends, sums, sizes):
    first, last = turn == 0, turn == len(TURNS) - 1
    nq = asked[0].shape[0] * (2 if first else 1)
    width = docs.shape[1]
    _, begin, end = TURNS[turn]
    nd = docs.shape[0] // len(SIDES) * (end - begin)
    vmem = pl.BlockSpec(memory_space=pltpu.VMEM)
    hbm = pl.BlockSpec(memory_space=pltpu.HBM)
    operands = [place, docs, *asked, ends, *sums]
    outs = nd // split
    out_shape = [pltpu.HBM((split, width), F32)] * outs
    out_shape += [jax.ShapeDtypeStruct((width, nq), F32), jax.ShapeDtypeStruct((8, width if last else nq), F32)]
    if first:
        line = jax.ShapeDtypeStruct((1, nq), F32)
        out_shape += [jax.ShapeDtypeStruct((nq, width), BF16), jax.ShapeDtypeStruct((width, nq), BF16)]
        out_shape += [line, line, jax.ShapeDtypeStruct((1, nq), jnp.int32)]
    return pl.pallas_call(
        functools.partial(kernel, sizes, turn, split),
        in_specs=[pl.BlockSpec(memory_space=pltpu.SMEM), vmem, hbm if first else vmem] + [vmem] * (len(operands) - 3),
        out_specs=[hbm] * outs + [vmem] * (len(out_shape) - outs),
        out_shape=out_shape,
        scratch_shapes=[
            pltpu.VMEM((width, nd), BF16),
            pltpu.VMEM((nd, 128), jnp.int32),
            pltpu.VMEM((2, nd, QT), BF16),
            pltpu.VMEM((nd, width), F32),
            pltpu.SemaphoreType.DMA((nd // SUB + 1,)),
        ],
        input_output_aliases={} if first else {8: outs},
        compiler_params=pltpu.CompilerParams(vmem_limit_bytes=VMEM_LIMIT),
        cost_estimate=pl.CostEstimate(flops=6 * nq * nd * width, bytes_accessed=8 << 20, transcendentals=nq * nd),
        name="fused",
    )(*operands)


def all_sides(array, along):
    return {side: moved(array, along, side) for side in (0, 2, 1, -1)}


def on_device(queries, documents, log_norms, weights, positives):
    own, width = queries.shape
    piece = documents.shape[0]
    total_q = own * lax.axis_size(AXES)
    n_x, n_y, n_z = lax.axis_size(X), lax.axis_size(Y), lax.axis_size("z")
    place = jnp.stack([lax.axis_index(X), lax.axis_index(Y), lax.axis_index("core")]).astype(jnp.int32)
    core = lax.axis_index("core")

    rows = jnp.stack([log_norms, weights, positives.astype(F32)])
    others = other_core(queries), other_core(rows)
    asked = (pltpu.with_memory_space_constraint(queries, pltpu.HBM), others[0], rows, others[1])

    column = lax.all_to_all(jnp.broadcast_to(documents[None], (n_z, piece, width)), "z", 0, 0, tiled=True)
    low, high = column.reshape(2, n_z // 2 * piece, width)
    mine, others = jnp.where(core == 0, low, high), jnp.where(core == 0, high, low)
    part = jnp.concatenate([mine, other_core(others)])
    near = all_sides(part, False)
    docs = all_sides(jnp.concatenate([near[s] for s in SIDES]), True)

    nd = docs[0].shape[0]
    terms = {}
    ends = (weights * log_norms).reshape(-1, width).sum(0)[None]
    sums = ()
    for turn, (side, begin, end) in enumerate(TURNS):
        count = nd // len(SIDES) * (end - begin)
        outs = 2 if side == 2 else 1
        got = fused(turn, count // outs, place, docs[side], asked, ends, sums, (n_x, n_y, n_z))
        terms.setdefault(side, []).extend(got[:outs])
        sums = grad_q, lost = got[outs : outs + 2]
        asked = got[outs + 2 :] or asked

    n = nd // 2
    far_a = moved(terms[2][0], True, -1)
    far_b = moved(terms[2][1], True, 1)
    behind = moved(jnp.concatenate([terms[-1][0][:n], terms[-1][0][n:] + far_b]), True, 1)
    ahead_a = moved(terms[1][0] + far_a, True, -1)
    ahead_b = moved(jnp.concatenate([terms[1][1], lost]), True, -1)
    lost = lost + moved(lost, True, 1) + moved(lost, True, 2) + ahead_b[n:]
    total = terms[0][0] + jnp.concatenate([ahead_a, ahead_b[:n]]) + behind
    n = nd // 4
    part = sum(
        moved(jnp.concatenate([total[i * n : (i + 1) * n], lost]), False, -s) for i, s in enumerate(SIDES)
    )
    mine, given = part[: n // 2], part[n // 2 :]
    got = other_core(given)
    lost = given[n // 2 :] + got[n // 2 :]
    got = got[: n // 2]
    low, high = jnp.where(core == 0, mine, got), jnp.where(core == 0, got, mine)
    part = jnp.concatenate([low, high]).reshape(n_z, piece, width)
    part = jnp.concatenate([part, jnp.broadcast_to(lost[None], (n_z, 8, width))], 1)
    part = lax.all_to_all(part, "z", 0, 0, tiled=True)
    part = part.sum(0)
    grad_documents = (part[:piece] * 0.0625).astype(BF16)
    loss = jnp.sum(part[piece:]) / total_q

    other_grad = grad_q[:, own:]
    other_grad = other_core(other_grad)
    grad_queries = ((grad_q[:, :own] + other_grad).T * 0.0625).astype(BF16)
    return (grad_queries, grad_documents, loss)


def solution(mesh):
    torus = Mesh(mesh.devices.reshape(8, 2, 2, 4, 2), AXES)
    placed = (P(AXES, None), P(AXES, None), P(AXES), P(AXES), P(AXES))
    return jax.shard_map(
        on_device,
        mesh=torus,
        in_specs=placed,
        out_specs=(P(AXES, None), P(AXES, None), P()),
        check_vma=False,
    )
```

```python
import functools
import itertools
import math

import jax
import jax.numpy as jnp
from jax import lax
from jax.experimental import pallas as pl
from jax.experimental.pallas import tpu as pltpu
from jax.sharding import Mesh
from jax.sharding import PartitionSpec as P


AXES = ("z", "xh", "core", "y", "xl")
X = ("xh", "xl")
Y = ("y",)
CHIPS = ("xh", "core", "y", "xl")
F32 = jnp.float32
BF16 = jnp.bfloat16
LOG2E = math.log2(math.e)
QT = 512
SUB = 256
SIDES = (0, 2, 1, -1)
TURNS = ((0, 0, 4), (2, 0, 4), (-1, 0, 4), (1, 0, 2), (1, 2, 4))
VMEM_LIMIT = 16 << 20


def other_core(array):
    return lax.ppermute(array, "core", [(0, 1), (1, 0)])


def moved(array, along, distance):
    if distance == 0:
        return array
    n_xh, n_y, n_xl = (lax.axis_size(axis) for axis in ("xh", "y", "xl"))
    n_x = n_xh * n_xl

    def at(x, core, y):
        return ((x // n_xl * 2 + core) * n_y + y) * n_xl + x % n_xl

    route = []
    for x, core, y in itertools.product(range(n_x), range(2), range(n_y)):
        in_x = along == (core == 0)
        to = ((x + distance) % n_x, y) if in_x else (x, (y + distance) % n_y)
        route.append((at(x, core, y), at(to[0], core, to[1])))
    return lax.ppermute(array, CHIPS, route)


def lay_out(own_ref, other_ref, rows_ref, other_rows_ref, q_ref, qt_ref, off_ref, w_ref, pos_ref, sem):
    n = own_ref.shape[0]
    own = pltpu.make_async_copy(own_ref, q_ref.at[:n], sem)
    own.start()
    for i, ref in enumerate((rows_ref, other_rows_ref)):
        part = slice(i * n, (i + 1) * n)
        w_ref[:, part] = ref[1:2, :]
        off_ref[:, part] = ref[0:1, :] * LOG2E - jnp.log2(ref[1:2, :])
        pos_ref[:, part] = ref[2:3, :].astype(jnp.int32)
    q_ref[n:, :] = other_ref[...]
    qt_ref[:, n:] = other_ref[...].T
    own.wait()
    qt_ref[:, :n] = q_ref[:n, :].T


def kernel(sizes, turn, split, *refs):
    n_x, n_y, n_z = sizes
    first, last = turn == 0, turn == len(TURNS) - 1
    side, begin, end = TURNS[turn]
    place_ref, d_ref, *refs = refs
    if first:
        given, ends_ref, refs = refs[:4], refs[4], refs[5:]
    else:
        q_ref, qt_ref, off_ref, w_ref, pos_ref, ends_ref, gq_in, found_in, *refs = refs
    piece = d_ref.shape[0] // (len(SIDES) * n_z)
    nd = (end - begin) * n_z * piece
    d_ref = d_ref.at[pl.ds(begin * n_z * piece, nd)]
    outs = nd // split
    gd_refs, refs = refs[:outs], refs[outs:]
    gq_ref, found_ref, *refs = refs
    if first:
        q_ref, qt_ref, off_ref, w_ref, pos_ref, *refs = refs
        lay_out(*given, q_ref, qt_ref, off_ref, w_ref, pos_ref, refs[-1].at[nd // SUB])
    nq = q_ref.shape[0]
    dt_ref, id_ref, c_ref, gd_ref, sems = refs

    if last:
        top = lax.broadcasted_iota(jnp.int32, found_ref.shape, 0) == 0
        found_ref[...] = jnp.where(top, ends_ref[...], 0.0)
    x, y, core = place_ref[0], place_ref[1], place_ref[2]
    row = lax.broadcasted_iota(jnp.int32, (piece, 128), 0)
    for step, across in enumerate(SIDES[begin:end]):
        from_x = (x - jnp.where(core == 0, side, across) + n_x) % n_x
        from_y = (y - jnp.where(core == 0, across, side) + n_y) % n_y
        for j in range(n_z):
            z = j % (n_z // 2) + core * (n_z // 2)
            owner = core if j < n_z // 2 else 1 - core
            base = ((z * 2 + from_x // 2) * 2 + owner) * 2 * n_y + from_y * 2 + from_x % 2
            at = (step * n_z + j) * piece
            id_ref[at : at + piece, :] = row + base * piece
    dt_ref[...] = d_ref[...].T

    def front(tile, slot):
        cols = pl.ds(pl.multiple_of(tile * QT, QT), QT)
        q_t = qt_ref[:, cols]
        off = off_ref[:, cols]
        w = w_ref[:, cols]
        pos = pos_ref[:, cols]
        found = jnp.zeros((8, QT), F32)
        for r in range(0, nd, SUB):
            scores = jnp.dot(d_ref[r : r + SUB, :], q_t, preferred_element_type=F32)
            probs = jnp.exp2(scores * (0.0625 * LOG2E) - off)
            hits = jnp.concatenate([id_ref[r : r + SUB, :]] * (QT // 128), 1) == pos
            c_ref[slot, r : r + SUB, :] = (probs - jnp.where(hits, w, 0.0)).astype(BF16)
            found = found + jnp.sum(jnp.where(hits, scores, 0.0).reshape(SUB // 8, 8, QT), 0)
        if not first:
            found = found_in[:, cols] + found
        if last:
            found = 0.0625 * w * found
            width = found_ref.shape[1]
            for c in range(0, QT, width):
                found_ref[...] -= found[:, c : c + width]
        else:
            found_ref[:, cols] = found

    def back(tile, slot, opening=False, closing=False):
        cols = pl.ds(pl.multiple_of(tile * QT, QT), QT)
        q = q_ref[cols, :]
        leave = []
        for r in range(0, nd, SUB):
            rows = slice(r, r + SUB)
            term = jnp.dot(c_ref[slot, rows, :], q, preferred_element_type=F32)
            gd_ref[rows, :] = term if opening else gd_ref[rows, :] + term
            if closing:
                out = gd_refs[r // split].at[pl.ds(r % split, SUB)]
                leave.append(pltpu.make_async_copy(gd_ref.at[rows], out, sems.at[r // SUB]))
                leave[-1].start()
        term = jnp.dot(dt_ref[...], c_ref[slot], preferred_element_type=F32)
        gq_ref[:, cols] = term if first else gq_in[:, cols] + term
        if closing and last:
            out = gd_refs[-1].at[pl.ds(split, found_ref.shape[0])]
            leave.append(pltpu.make_async_copy(found_ref, out, sems.at[nd // SUB]))
            leave[-1].start()
        for copy in leave:
            copy.wait()

    tiles = nq // QT
    front(0, 0)
    front(1, 1)
    back(0, 0, opening=True)

    def pair(i, _):
        tile = 2 * i + 1
        front(tile + 1, 0)
        back(tile, 1)
        front(tile + 2, 1)
        back(tile + 1, 0)
        return 0

    lax.fori_loop(0, (tiles - 2) // 2, pair, 0)
    back(tiles - 1, 1, closing=True)


def fused(turn, split, place, docs, asked, ends, sums, sizes):
    first, last = turn == 0, turn == len(TURNS) - 1
    nq = asked[0].shape[0] * (2 if first else 1)
    width = docs.shape[1]
    _, begin, end = TURNS[turn]
    nd = docs.shape[0] // len(SIDES) * (end - begin)
    vmem = pl.BlockSpec(memory_space=pltpu.VMEM)
    hbm = pl.BlockSpec(memory_space=pltpu.HBM)
    operands = [place, docs, *asked, ends, *sums]
    outs = nd // split
    out_shape = [pltpu.HBM((split + 8 if last else split, width), F32)] * outs
    out_shape += [jax.ShapeDtypeStruct((width, nq), F32), jax.ShapeDtypeStruct((8, width if last else nq), F32)]
    if first:
        line = jax.ShapeDtypeStruct((1, nq), F32)
        out_shape += [jax.ShapeDtypeStruct((nq, width), BF16), jax.ShapeDtypeStruct((width, nq), BF16)]
        out_shape += [line, line, jax.ShapeDtypeStruct((1, nq), jnp.int32)]
    return pl.pallas_call(
        functools.partial(kernel, sizes, turn, split),
        in_specs=[pl.BlockSpec(memory_space=pltpu.SMEM), vmem, hbm if first else vmem] + [vmem] * (len(operands) - 3),
        out_specs=[hbm] * outs + [vmem] * (len(out_shape) - outs),
        out_shape=out_shape,
        scratch_shapes=[
            pltpu.VMEM((width, nd), BF16),
            pltpu.VMEM((nd, 128), jnp.int32),
            pltpu.VMEM((2, nd, QT), BF16),
            pltpu.VMEM((nd, width), F32),
            pltpu.SemaphoreType.DMA((nd // SUB + 1,)),
        ],
        input_output_aliases={} if first else {8: outs},
        compiler_params=pltpu.CompilerParams(vmem_limit_bytes=VMEM_LIMIT),
        cost_estimate=pl.CostEstimate(flops=6 * nq * nd * width, bytes_accessed=8 << 20, transcendentals=nq * nd),
        name="fused",
    )(*operands)


def all_sides(array, along):
    return {side: moved(array, along, side) for side in (0, 2, 1, -1)}


def on_device(queries, documents, log_norms, weights, positives):
    own, width = queries.shape
    piece = documents.shape[0]
    total_q = own * lax.axis_size(AXES)
    n_x, n_y, n_z = lax.axis_size(X), lax.axis_size(Y), lax.axis_size("z")
    place = jnp.stack([lax.axis_index(X), lax.axis_index(Y), lax.axis_index("core")]).astype(jnp.int32)
    core = lax.axis_index("core")

    rows = jnp.stack([log_norms, weights, positives.astype(F32)])
    others = other_core(queries), other_core(rows)
    asked = (pltpu.with_memory_space_constraint(queries, pltpu.HBM), others[0], rows, others[1])

    column = lax.all_to_all(jnp.broadcast_to(documents[None], (n_z, piece, width)), "z", 0, 0, tiled=True)
    low, high = column.reshape(2, n_z // 2 * piece, width)
    mine, others = jnp.where(core == 0, low, high), jnp.where(core == 0, high, low)
    part = jnp.concatenate([mine, other_core(others)])
    near = all_sides(part, False)
    docs = all_sides(jnp.concatenate([near[s] for s in SIDES]), True)

    nd = docs[0].shape[0]
    terms = {}
    ends = (weights * log_norms).reshape(-1, width).sum(0)[None]
    sums = ()
    for turn, (side, begin, end) in enumerate(TURNS):
        count = nd // len(SIDES) * (end - begin)
        outs = count * 2 // nd
        got = fused(turn, count // outs, place, docs[side], asked, ends, sums, (n_x, n_y, n_z))
        terms.setdefault(side, []).extend(got[:outs])
        sums = grad_q, lost = got[outs : outs + 2]
        asked = got[outs + 2 :] or asked

    n = nd // 2
    far_a = moved(terms[2][0], True, -1)
    far_b = moved(terms[2][1], True, 1)
    behind_a = moved(terms[-1][0], True, 1)
    behind_b = moved(terms[-1][1] + far_b, True, 1)
    ahead_a = moved(terms[1][0] + far_a, True, -1)
    ahead_b = moved(terms[1][1], True, -1)
    lost = lost + moved(lost, True, 1) + moved(lost, True, 2) + ahead_b[n:]
    near = terms[0][0] + ahead_a + behind_a
    next_to = terms[0][1] + ahead_b[:n] + behind_b
    n = nd // 4
    opposite = moved(near[n:], False, -2)
    one = moved(jnp.concatenate([next_to[:n], lost]), False, -1)
    other = moved(jnp.concatenate([next_to[n:], lost]), False, 1)
    lost = lost + moved(lost, False, 2) + one[n:] + other[n:]
    part = near[:n] + opposite + one[:n] + other[:n]
    mine, given = part[: n // 2], part[n // 2 :]
    got = other_core(jnp.concatenate([given, lost]))
    lost = lost + got[n // 2 :]
    got = got[: n // 2]
    low, high = jnp.where(core == 0, mine, got), jnp.where(core == 0, got, mine)
    part = jnp.concatenate([low, high]).reshape(n_z, piece, width)
    part = jnp.concatenate([part, jnp.broadcast_to(lost[None], (n_z, 8, width))], 1)
    part = lax.all_to_all(part, "z", 0, 0, tiled=True)
    part = part.sum(0)
    grad_documents = (part[:piece] * 0.0625).astype(BF16)
    loss = jnp.sum(part[piece:]) / total_q

    other_grad = grad_q[:, own:]
    other_grad = other_core(other_grad)
    grad_queries = ((grad_q[:, :own] + other_grad).T * 0.0625).astype(BF16)
    return (grad_queries, grad_documents, loss)


def solution(mesh):
    torus = Mesh(mesh.devices.reshape(8, 2, 2, 4, 2), AXES)
    placed = (P(AXES, None), P(AXES, None), P(AXES), P(AXES), P(AXES))
    return jax.shard_map(
        on_device,
        mesh=torus,
        in_specs=placed,
        out_specs=(P(AXES, None), P(AXES, None), P()),
        check_vma=False,
    )
```

```python
import functools
import itertools
import math

import jax
import jax.numpy as jnp
from jax import lax
from jax.experimental import pallas as pl
from jax.experimental.pallas import tpu as pltpu
from jax.sharding import Mesh
from jax.sharding import PartitionSpec as P


AXES = ("z", "xh", "core", "y", "xl")
X = ("xh", "xl")
Y = ("y",)
CHIPS = ("xh", "core", "y", "xl")
F32 = jnp.float32
BF16 = jnp.bfloat16
LOG2E = math.log2(math.e)
QT = 512
SUB = 256
SIDES = (0, 1, -1, 2)
TURNS = ((0, 0, 4), (2, 0, 4), (-1, 0, 4), (1, 0, 2), (1, 2, 4))
VMEM_LIMIT = 16 << 20


def other_core(array):
    return lax.ppermute(array, "core", [(0, 1), (1, 0)])


def moved(array, along, distance):
    if distance == 0:
        return array
    n_xh, n_y, n_xl = (lax.axis_size(axis) for axis in ("xh", "y", "xl"))
    n_x = n_xh * n_xl

    def at(x, core, y):
        return ((x // n_xl * 2 + core) * n_y + y) * n_xl + x % n_xl

    route = []
    for x, core, y in itertools.product(range(n_x), range(2), range(n_y)):
        in_x = along == (core == 0)
        to = ((x + distance) % n_x, y) if in_x else (x, (y + distance) % n_y)
        route.append((at(x, core, y), at(to[0], core, to[1])))
    return lax.ppermute(array, CHIPS, route)


def lay_out(own_ref, other_ref, rows_ref, other_rows_ref, q_ref, qt_ref, off_ref, w_ref, pos_ref, sem):
    n = own_ref.shape[0]
    own = pltpu.make_async_copy(own_ref, q_ref.at[:n], sem)
    own.start()
    for i, ref in enumerate((rows_ref, other_rows_ref)):
        part = slice(i * n, (i + 1) * n)
        w_ref[:, part] = ref[1:2, :]
        off_ref[:, part] = ref[0:1, :] * LOG2E - jnp.log2(ref[1:2, :])
        pos_ref[:, part] = ref[2:3, :].astype(jnp.int32)
    q_ref[n:, :] = other_ref[...]
    qt_ref[:, n:] = other_ref[...].T
    own.wait()
    qt_ref[:, :n] = q_ref[:n, :].T


def kernel(sizes, turn, split, *refs):
    n_x, n_y, n_z = sizes
    first, last = turn == 0, turn == len(TURNS) - 1
    side, begin, end = TURNS[turn]
    place_ref, d_ref, *refs = refs
    if first:
        given, ends_ref, refs = refs[:4], refs[4], refs[5:]
    else:
        q_ref, qt_ref, off_ref, w_ref, pos_ref, ends_ref, gq_in, found_in, *refs = refs
    piece = d_ref.shape[0] // (len(SIDES) * n_z)
    nd = (end - begin) * n_z * piece
    d_ref = d_ref.at[pl.ds(begin * n_z * piece, nd)]
    outs = nd // split
    gd_refs, refs = refs[:outs], refs[outs:]
    gq_ref, found_ref, *refs = refs
    if first:
        q_ref, qt_ref, off_ref, w_ref, pos_ref, *refs = refs
        lay_out(*given, q_ref, qt_ref, off_ref, w_ref, pos_ref, refs[-1].at[nd // SUB])
    nq = q_ref.shape[0]
    dt_ref, id_ref, c_ref, gd_ref, sems = refs

    if last:
        top = lax.broadcasted_iota(jnp.int32, found_ref.shape, 0) == 0
        found_ref[...] = jnp.where(top, ends_ref[...], 0.0)
    x, y, core = place_ref[0], place_ref[1], place_ref[2]
    row = lax.broadcasted_iota(jnp.int32, (piece, 128), 0)
    for step, across in enumerate(SIDES[begin:end]):
        from_x = (x - jnp.where(core == 0, side, across) + n_x) % n_x
        from_y = (y - jnp.where(core == 0, across, side) + n_y) % n_y
        for j in range(n_z):
            z = j % (n_z // 2) + core * (n_z // 2)
            owner = core if j < n_z // 2 else 1 - core
            base = ((z * 2 + from_x // 2) * 2 + owner) * 2 * n_y + from_y * 2 + from_x % 2
            at = (step * n_z + j) * piece
            id_ref[at : at + piece, :] = row + base * piece
    dt_ref[...] = d_ref[...].T

    def front(tile, slot):
        cols = pl.ds(pl.multiple_of(tile * QT, QT), QT)
        q_t = qt_ref[:, cols]
        off = off_ref[:, cols]
        w = w_ref[:, cols]
        pos = pos_ref[:, cols]
        found = jnp.zeros((8, QT), F32)
        for r in range(0, nd, SUB):
            scores = jnp.dot(d_ref[r : r + SUB, :], q_t, preferred_element_type=F32)
            probs = jnp.exp2(scores * (0.0625 * LOG2E) - off)
            hits = jnp.concatenate([id_ref[r : r + SUB, :]] * (QT // 128), 1) == pos
            c_ref[slot, r : r + SUB, :] = (probs - jnp.where(hits, w, 0.0)).astype(BF16)
            found = found + jnp.sum(jnp.where(hits, scores, 0.0).reshape(SUB // 8, 8, QT), 0)
        if not first:
            found = found_in[:, cols] + found
        if last:
            found = 0.0625 * w * found
            width = found_ref.shape[1]
            for c in range(0, QT, width):
                found_ref[...] -= found[:, c : c + width]
        else:
            found_ref[:, cols] = found

    def back(tile, slot, opening=False, closing=False):
        cols = pl.ds(pl.multiple_of(tile * QT, QT), QT)
        q = q_ref[cols, :]
        leave = []
        for r in range(0, nd, SUB):
            rows = slice(r, r + SUB)
            term = jnp.dot(c_ref[slot, rows, :], q, preferred_element_type=F32)
            gd_ref[rows, :] = term if opening else gd_ref[rows, :] + term
            if closing:
                out = gd_refs[r // split].at[pl.ds(r % split, SUB)]
                leave.append(pltpu.make_async_copy(gd_ref.at[rows], out, sems.at[r // SUB]))
                leave[-1].start()
        term = jnp.dot(dt_ref[...], c_ref[slot], preferred_element_type=F32)
        gq_ref[:, cols] = term if first else gq_in[:, cols] + term
        if closing and last:
            out = gd_refs[-1].at[pl.ds(split, found_ref.shape[0])]
            leave.append(pltpu.make_async_copy(found_ref, out, sems.at[nd // SUB]))
            leave[-1].start()
        for copy in leave:
            copy.wait()

    tiles = nq // QT
    front(0, 0)
    front(1, 1)
    back(0, 0, opening=True)

    def pair(i, _):
        tile = 2 * i + 1
        front(tile + 1, 0)
        back(tile, 1)
        front(tile + 2, 1)
        back(tile + 1, 0)
        return 0

    lax.fori_loop(0, (tiles - 2) // 2, pair, 0)
    back(tiles - 1, 1, closing=True)


def fused(turn, split, place, docs, asked, ends, sums, sizes):
    first, last = turn == 0, turn == len(TURNS) - 1
    nq = asked[0].shape[0] * (2 if first else 1)
    width = docs.shape[1]
    _, begin, end = TURNS[turn]
    nd = docs.shape[0] // len(SIDES) * (end - begin)
    vmem = pl.BlockSpec(memory_space=pltpu.VMEM)
    hbm = pl.BlockSpec(memory_space=pltpu.HBM)
    operands = [place, docs, *asked, ends, *sums]
    outs = nd // split
    out_shape = [pltpu.HBM((split + 8 if last else split, width), F32)] * outs
    out_shape += [jax.ShapeDtypeStruct((width, nq), F32), jax.ShapeDtypeStruct((8, width if last else nq), F32)]
    if first:
        line = jax.ShapeDtypeStruct((1, nq), F32)
        out_shape += [jax.ShapeDtypeStruct((nq, width), BF16), jax.ShapeDtypeStruct((width, nq), BF16)]
        out_shape += [line, line, jax.ShapeDtypeStruct((1, nq), jnp.int32)]
    return pl.pallas_call(
        functools.partial(kernel, sizes, turn, split),
        in_specs=[pl.BlockSpec(memory_space=pltpu.SMEM), vmem, hbm if first else vmem] + [vmem] * (len(operands) - 3),
        out_specs=[hbm] * outs + [vmem] * (len(out_shape) - outs),
        out_shape=out_shape,
        scratch_shapes=[
            pltpu.VMEM((width, nd), BF16),
            pltpu.VMEM((nd, 128), jnp.int32),
            pltpu.VMEM((2, nd, QT), BF16),
            pltpu.VMEM((nd, width), F32),
            pltpu.SemaphoreType.DMA((nd // SUB + 1,)),
        ],
        input_output_aliases={} if first else {8: outs},
        compiler_params=pltpu.CompilerParams(vmem_limit_bytes=VMEM_LIMIT),
        cost_estimate=pl.CostEstimate(flops=6 * nq * nd * width, bytes_accessed=8 << 20, transcendentals=nq * nd),
        name="fused",
    )(*operands)


def all_sides(array, along):
    sides = {}
    for side in (0, 2, 1, -1):
        sides[side] = moved(array, along, side)
    return sides


def on_device(queries, documents, log_norms, weights, positives):
    own, width = queries.shape
    piece = documents.shape[0]
    total_q = own * lax.axis_size(AXES)
    n_x, n_y, n_z = lax.axis_size(X), lax.axis_size(Y), lax.axis_size("z")
    place = jnp.stack([lax.axis_index(X), lax.axis_index(Y), lax.axis_index("core")]).astype(jnp.int32)
    core = lax.axis_index("core")

    rows = jnp.stack([log_norms, weights, positives.astype(F32)])
    others = other_core(queries), other_core(rows)
    asked = (pltpu.with_memory_space_constraint(queries, pltpu.HBM), others[0], rows, others[1])

    column = lax.all_to_all(jnp.broadcast_to(documents[None], (n_z, piece, width)), "z", 0, 0, tiled=True)
    low, high = column.reshape(2, n_z // 2 * piece, width)
    mine, others = jnp.where(core == 0, low, high), jnp.where(core == 0, high, low)
    part = jnp.concatenate([mine, other_core(others)])
    near = all_sides(part, False)
    docs = all_sides(jnp.concatenate([near[s] for s in SIDES]), True)

    nd = docs[0].shape[0]
    terms = {}
    ends = (weights * log_norms).reshape(-1, width).sum(0)[None]
    sums = ()
    for turn, (side, begin, end) in enumerate(TURNS):
        count = nd // len(SIDES) * (end - begin)
        outs = 2 if side == 2 else 1
        got = fused(turn, count // outs, place, docs[side], asked, ends, sums, (n_x, n_y, n_z))
        terms.setdefault(side, []).extend(got[:outs])
        sums = grad_q, lost = got[outs : outs + 2]
        asked = got[outs + 2 :] or asked

    n = nd // 2
    far_a = moved(terms[2][0], True, -1)
    far_b = moved(terms[2][1], True, 1)
    behind = moved(jnp.concatenate([terms[-1][0][:n], terms[-1][0][n:] + far_b]), True, 1)
    ahead_a = moved(terms[1][0] + far_a, True, -1)
    ahead_b = moved(terms[1][1], True, -1)
    lost = lost + moved(lost, True, 1) + moved(lost, True, 2) + ahead_b[n:]
    total = terms[0][0] + jnp.concatenate([ahead_a, ahead_b[:n]]) + behind
    n = nd // 4
    part = jnp.concatenate([total[:n], lost])
    for i, side in enumerate(SIDES):
        if side:
            part = part + moved(jnp.concatenate([total[i * n : (i + 1) * n], lost]), False, -side)
    mine, given = part[: n // 2], part[n // 2 :]
    got = other_core(given)
    lost = given[n // 2 :] + got[n // 2 :]
    got = got[: n // 2]
    low, high = jnp.where(core == 0, mine, got), jnp.where(core == 0, got, mine)
    part = jnp.concatenate([low, high]).reshape(n_z, piece, width)
    part = jnp.concatenate([part, jnp.broadcast_to(lost[None], (n_z, 8, width))], 1)
    part = lax.all_to_all(part, "z", 0, 0, tiled=True)
    part = part.sum(0)
    grad_documents = (part[:piece] * 0.0625).astype(BF16)
    loss = jnp.sum(part[piece:]) / total_q

    other_grad = grad_q[:, own:]
    other_grad = other_core(other_grad)
    grad_queries = ((grad_q[:, :own] + other_grad).T * 0.0625).astype(BF16)
    return (grad_queries, grad_documents, loss)


def solution(mesh):
    torus = Mesh(mesh.devices.reshape(8, 2, 2, 4, 2), AXES)
    placed = (P(AXES, None), P(AXES, None), P(AXES), P(AXES), P(AXES))
    return jax.shard_map(
        on_device,
        mesh=torus,
        in_specs=placed,
        out_specs=(P(AXES, None), P(AXES, None), P()),
        check_vma=False,
    )
```

```python
import functools
import itertools
import math

import jax
import jax.numpy as jnp
from jax import lax
from jax.experimental import pallas as pl
from jax.experimental.pallas import tpu as pltpu
from jax.sharding import Mesh
from jax.sharding import PartitionSpec as P


AXES = ("z", "xh", "core", "y", "xl")
X = ("xh", "xl")
Y = ("y",)
CHIPS = ("xh", "core", "y", "xl")
F32 = jnp.float32
BF16 = jnp.bfloat16
LOG2E = math.log2(math.e)
QT = 512
SUB = 256
SIDES = (0, 1, -1, 2)
TURNS = ((0, 0, 4), (2, 0, 4), (-1, 0, 4), (1, 0, 2), (1, 2, 4))
KEPT = 3
VMEM_LIMIT = 16 << 20


def other_core(array):
    return lax.ppermute(array, "core", [(0, 1), (1, 0)])


def moved(array, along, distance):
    if distance == 0:
        return array
    n_xh, n_y, n_xl = (lax.axis_size(axis) for axis in ("xh", "y", "xl"))
    n_x = n_xh * n_xl

    def at(x, core, y):
        return ((x // n_xl * 2 + core) * n_y + y) * n_xl + x % n_xl

    route = []
    for x, core, y in itertools.product(range(n_x), range(2), range(n_y)):
        in_x = along == (core == 0)
        to = ((x + distance) % n_x, y) if in_x else (x, (y + distance) % n_y)
        route.append((at(x, core, y), at(to[0], core, to[1])))
    return lax.ppermute(array, CHIPS, route)


def lay_out(own_ref, other_ref, rows_ref, other_rows_ref, q_ref, qt_ref, off_ref, w_ref, pos_ref, sem):
    n = own_ref.shape[0]
    own = pltpu.make_async_copy(own_ref, q_ref.at[:n], sem)
    own.start()
    for i, ref in enumerate((rows_ref, other_rows_ref)):
        part = slice(i * n, (i + 1) * n)
        w_ref[:, part] = ref[1:2, :]
        off_ref[:, part] = ref[0:1, :] * LOG2E - jnp.log2(ref[1:2, :])
        pos_ref[:, part] = ref[2:3, :].astype(jnp.int32)
    q_ref[n:, :] = other_ref[...]
    qt_ref[:, n:] = other_ref[...].T
    own.wait()
    qt_ref[:, :n] = q_ref[:n, :].T


def kernel(sizes, turn, split, *refs):
    n_x, n_y, n_z = sizes
    first, last = turn == 0, turn == len(TURNS) - 1
    kept = turn >= KEPT
    side, begin, end = TURNS[turn]
    place_ref, d_ref, *refs = refs
    if first:
        given, ends_ref, refs = refs[:4], refs[4], refs[5:]
    else:
        q_ref, qt_ref, off_ref, w_ref, pos_ref, ends_ref, gq_in, found_in, *refs = refs
    piece = d_ref.shape[0] // (len(SIDES) * n_z)
    nd = (end - begin) * n_z * piece
    d_ref = d_ref.at[pl.ds(begin * n_z * piece, nd)]
    outs = nd // split
    gd_refs, refs = refs[:outs], refs[outs:]
    gq_ref, found_ref, *refs = refs
    if first:
        q_ref, qt_ref, off_ref, w_ref, pos_ref, *refs = refs
        lay_out(*given, q_ref, qt_ref, off_ref, w_ref, pos_ref, refs[-1].at[nd // SUB])
    nq = q_ref.shape[0]
    dt_ref, id_ref, c_ref, gd_ref, sems = refs

    if last:
        top = lax.broadcasted_iota(jnp.int32, found_ref.shape, 0) == 0
        found_ref[...] = jnp.where(top, ends_ref[...], 0.0)
    x, y, core = place_ref[0], place_ref[1], place_ref[2]
    row = lax.broadcasted_iota(jnp.int32, (piece, 128), 0)
    for step, across in enumerate(SIDES[begin:end]):
        from_x = (x - jnp.where(core == 0, side, across) + n_x) % n_x
        from_y = (y - jnp.where(core == 0, across, side) + n_y) % n_y
        for j in range(n_z):
            z = j % (n_z // 2) + core * (n_z // 2)
            owner = core if j < n_z // 2 else 1 - core
            base = ((z * 2 + from_x // 2) * 2 + owner) * 2 * n_y + from_y * 2 + from_x % 2
            at = (step * n_z + j) * piece
            id_ref[at : at + piece, :] = row + base * piece
    dt_ref[...] = d_ref[...].T

    def front(tile, slot):
        cols = pl.ds(pl.multiple_of(tile * QT, QT), QT)
        q_t = qt_ref[:, cols]
        off = off_ref[:, cols]
        w = w_ref[:, cols]
        pos = pos_ref[:, cols]
        found = jnp.zeros((8, QT), F32)
        for r in range(0, nd, SUB):
            scores = jnp.dot(d_ref[r : r + SUB, :], q_t, preferred_element_type=F32)
            probs = jnp.exp2(scores * (0.0625 * LOG2E) - off)
            hits = jnp.concatenate([id_ref[r : r + SUB, :]] * (QT // 128), 1) == pos
            c_ref[slot, r : r + SUB, :] = (probs - jnp.where(hits, w, 0.0)).astype(BF16)
            found = found + jnp.sum(jnp.where(hits, scores, 0.0).reshape(SUB // 8, 8, QT), 0)
        if not first:
            found = found_in[:, cols] + found
        if last:
            found = 0.0625 * w * found
            width = found_ref.shape[1]
            for c in range(0, QT, width):
                found_ref[...] -= found[:, c : c + width]
        else:
            found_ref[:, cols] = found

    def back(tile, slot, opening=False, closing=False):
        cols = pl.ds(pl.multiple_of(tile * QT, QT), QT)
        q = q_ref[cols, :]
        leave = []
        for r in range(0, nd, SUB):
            rows = slice(r, r + SUB)
            term = jnp.dot(c_ref[slot, rows, :], q, preferred_element_type=F32)
            if not opening:
                term = gd_ref[rows, :] + term
            if closing and kept:
                gd_refs[r // split][r % split : r % split + SUB, :] = term
            else:
                gd_ref[rows, :] = term
            if closing and not kept:
                out = gd_refs[r // split].at[pl.ds(r % split, SUB)]
                leave.append(pltpu.make_async_copy(gd_ref.at[rows], out, sems.at[r // SUB]))
                leave[-1].start()
        term = jnp.dot(dt_ref[...], c_ref[slot], preferred_element_type=F32)
        gq_ref[:, cols] = term if first else gq_in[:, cols] + term
        if closing and last:
            gd_refs[-1][split:, :] = found_ref[...]
        for copy in leave:
            copy.wait()

    tiles = nq // QT
    front(0, 0)
    front(1, 1)
    back(0, 0, opening=True)

    def pair(i, _):
        tile = 2 * i + 1
        front(tile + 1, 0)
        back(tile, 1)
        front(tile + 2, 1)
        back(tile + 1, 0)
        return 0

    lax.fori_loop(0, (tiles - 2) // 2, pair, 0)
    back(tiles - 1, 1, closing=True)


def fused(turn, split, place, docs, asked, ends, sums, sizes):
    first, last = turn == 0, turn == len(TURNS) - 1
    nq = asked[0].shape[0] * (2 if first else 1)
    width = docs.shape[1]
    _, begin, end = TURNS[turn]
    nd = docs.shape[0] // len(SIDES) * (end - begin)
    vmem = pl.BlockSpec(memory_space=pltpu.VMEM)
    hbm = pl.BlockSpec(memory_space=pltpu.HBM)
    operands = [place, docs, *asked, ends, *sums]
    outs = nd // split
    kept = turn >= KEPT
    sums_shape = (split + 8 if last else split, width)
    out_shape = [jax.ShapeDtypeStruct(sums_shape, F32) if kept else pltpu.HBM(sums_shape, F32)] * outs
    out_shape += [jax.ShapeDtypeStruct((width, nq), F32), jax.ShapeDtypeStruct((8, width if last else nq), F32)]
    if first:
        line = jax.ShapeDtypeStruct((1, nq), F32)
        out_shape += [jax.ShapeDtypeStruct((nq, width), BF16), jax.ShapeDtypeStruct((width, nq), BF16)]
        out_shape += [line, line, jax.ShapeDtypeStruct((1, nq), jnp.int32)]
    return pl.pallas_call(
        functools.partial(kernel, sizes, turn, split),
        in_specs=[pl.BlockSpec(memory_space=pltpu.SMEM), vmem, hbm if first else vmem] + [vmem] * (len(operands) - 3),
        out_specs=[vmem if kept else hbm] * outs + [vmem] * (len(out_shape) - outs),
        out_shape=out_shape,
        scratch_shapes=[
            pltpu.VMEM((width, nd), BF16),
            pltpu.VMEM((nd, 128), jnp.int32),
            pltpu.VMEM((2, nd, QT), BF16),
            pltpu.VMEM((nd, width), F32),
            pltpu.SemaphoreType.DMA((nd // SUB + 1,)),
        ],
        input_output_aliases={} if first else {8: outs},
        compiler_params=pltpu.CompilerParams(vmem_limit_bytes=VMEM_LIMIT),
        cost_estimate=pl.CostEstimate(flops=6 * nq * nd * width, bytes_accessed=8 << 20, transcendentals=nq * nd),
        name="fused",
    )(*operands)


def all_sides(array, along):
    sides = {}
    for side in (0, 2, 1, -1):
        sides[side] = moved(array, along, side)
    return sides


def on_device(queries, documents, log_norms, weights, positives):
    own, width = queries.shape
    piece = documents.shape[0]
    total_q = own * lax.axis_size(AXES)
    n_x, n_y, n_z = lax.axis_size(X), lax.axis_size(Y), lax.axis_size("z")
    place = jnp.stack([lax.axis_index(X), lax.axis_index(Y), lax.axis_index("core")]).astype(jnp.int32)
    core = lax.axis_index("core")

    rows = jnp.stack([log_norms, weights, positives.astype(F32)])
    others = other_core(queries), other_core(rows)
    asked = (pltpu.with_memory_space_constraint(queries, pltpu.HBM), others[0], rows, others[1])

    column = lax.all_to_all(jnp.broadcast_to(documents[None], (n_z, piece, width)), "z", 0, 0, tiled=True)
    low, high = column.reshape(2, n_z // 2 * piece, width)
    mine, others = jnp.where(core == 0, low, high), jnp.where(core == 0, high, low)
    part = jnp.concatenate([mine, other_core(others)])
    near = all_sides(part, False)
    docs = all_sides(jnp.concatenate([near[s] for s in SIDES]), True)

    nd = docs[0].shape[0]
    terms = {}
    ends = (weights * log_norms).reshape(-1, width).sum(0)[None]
    sums = ()
    for turn, (side, begin, end) in enumerate(TURNS):
        count = nd // len(SIDES) * (end - begin)
        outs = 2 if side == 2 else 1
        got = fused(turn, count // outs, place, docs[side], asked, ends, sums, (n_x, n_y, n_z))
        terms.setdefault(side, []).extend(got[:outs])
        sums = grad_q, lost = got[outs : outs + 2]
        asked = got[outs + 2 :] or asked

    n = nd // 2
    far_a = moved(terms[2][0], True, -1)
    far_b = moved(terms[2][1], True, 1)
    behind = moved(jnp.concatenate([terms[-1][0][:n], terms[-1][0][n:] + far_b]), True, 1)
    ahead_a = moved(terms[1][0] + far_a, True, -1)
    ahead_b = moved(terms[1][1], True, -1)
    lost = lost + moved(lost, True, 1) + moved(lost, True, 2) + ahead_b[n:]
    total = terms[0][0] + jnp.concatenate([ahead_a, ahead_b[:n]]) + behind
    n = nd // 4
    part = jnp.concatenate([total[:n], lost])
    for i, side in enumerate(SIDES):
        if side:
            part = part + moved(jnp.concatenate([total[i * n : (i + 1) * n], lost]), False, -side)
    mine, given = part[: n // 2], part[n // 2 :]
    got = other_core(given)
    lost = given[n // 2 :] + got[n // 2 :]
    got = got[: n // 2]
    low, high = jnp.where(core == 0, mine, got), jnp.where(core == 0, got, mine)
    part = jnp.concatenate([low, high]).reshape(n_z, piece, width)
    part = jnp.concatenate([part, jnp.broadcast_to(lost[None], (n_z, 8, width))], 1)
    part = lax.all_to_all(part, "z", 0, 0, tiled=True)
    part = part.sum(0)
    grad_documents = (part[:piece] * 0.0625).astype(BF16)
    loss = jnp.sum(part[piece:]) / total_q

    other_grad = grad_q[:, own:]
    other_grad = other_core(other_grad)
    grad_queries = ((grad_q[:, :own] + other_grad).T * 0.0625).astype(BF16)
    return (grad_queries, grad_documents, loss)


def solution(mesh):
    torus = Mesh(mesh.devices.reshape(8, 2, 2, 4, 2), AXES)
    placed = (P(AXES, None), P(AXES, None), P(AXES), P(AXES), P(AXES))
    return jax.shard_map(
        on_device,
        mesh=torus,
        in_specs=placed,
        out_specs=(P(AXES, None), P(AXES, None), P()),
        check_vma=False,
    )
```

```python
import functools
import itertools
import math

import jax
import jax.numpy as jnp
from jax import lax
from jax.experimental import pallas as pl
from jax.experimental.pallas import tpu as pltpu
from jax.sharding import Mesh
from jax.sharding import PartitionSpec as P


AXES = ("z", "xh", "core", "y", "xl")
X = ("xh", "xl")
Y = ("y",)
CHIPS = ("xh", "core", "y", "xl")
F32 = jnp.float32
BF16 = jnp.bfloat16
LOG2E = math.log2(math.e)
QT = 512
SUB = 256
SIDES = (0, 1, -1, 2)
TURNS = ((0, 0, 4), (2, 0, 4), (-1, 0, 4), (1, 0, 2), (1, 2, 4))
KEPT = 3
VMEM_LIMIT = 16 << 20


def other_core(array):
    return lax.ppermute(array, "core", [(0, 1), (1, 0)])


def moved(array, along, distance):
    if distance == 0:
        return array
    n_xh, n_y, n_xl = (lax.axis_size(axis) for axis in ("xh", "y", "xl"))
    n_x = n_xh * n_xl

    def at(x, core, y):
        return ((x // n_xl * 2 + core) * n_y + y) * n_xl + x % n_xl

    route = []
    for x, core, y in itertools.product(range(n_x), range(2), range(n_y)):
        in_x = along == (core == 0)
        to = ((x + distance) % n_x, y) if in_x else (x, (y + distance) % n_y)
        route.append((at(x, core, y), at(to[0], core, to[1])))
    return lax.ppermute(array, CHIPS, route)


def lay_out(own_ref, other_ref, rows_ref, other_rows_ref, q_ref, qt_ref, off_ref, w_ref, pos_ref, sem):
    n = own_ref.shape[0]
    own = pltpu.make_async_copy(own_ref, q_ref.at[:n], sem)
    own.start()
    for i, ref in enumerate((rows_ref, other_rows_ref)):
        part = slice(i * n, (i + 1) * n)
        w_ref[:, part] = ref[1:2, :]
        off_ref[:, part] = ref[0:1, :] * LOG2E - jnp.log2(ref[1:2, :])
        pos_ref[:, part] = ref[2:3, :].astype(jnp.int32)
    q_ref[n:, :] = other_ref[...]
    qt_ref[:, n:] = other_ref[...].T
    own.wait()
    qt_ref[:, :n] = q_ref[:n, :].T


def kernel(sizes, turn, split, *refs):
    n_x, n_y, n_z = sizes
    first, last = turn == 0, turn == len(TURNS) - 1
    kept = turn >= KEPT
    side, begin, end = TURNS[turn]
    place_ref, d_ref, *refs = refs
    if first:
        given, ends_ref, refs = refs[:4], refs[4], refs[5:]
    else:
        q_ref, qt_ref, off_ref, w_ref, pos_ref, ends_ref, gq_in, found_in, *refs = refs
    piece = d_ref.shape[0] // (len(SIDES) * n_z)
    nd = (end - begin) * n_z * piece
    d_ref = d_ref.at[pl.ds(begin * n_z * piece, nd)]
    outs = nd // split
    gd_refs, refs = refs[:outs], refs[outs:]
    gq_ref, found_ref, *refs = refs
    if first:
        q_ref, qt_ref, off_ref, w_ref, pos_ref, *refs = refs
        lay_out(*given, q_ref, qt_ref, off_ref, w_ref, pos_ref, refs[-1].at[nd // SUB])
    nq = q_ref.shape[0]
    dt_ref, id_ref, c_ref, gd_ref, sems = refs

    if last:
        top = lax.broadcasted_iota(jnp.int32, found_ref.shape, 0) == 0
        found_ref[...] = jnp.where(top, ends_ref[...], 0.0)
    x, y, core = place_ref[0], place_ref[1], place_ref[2]
    row = lax.broadcasted_iota(jnp.int32, (piece, 128), 0)
    for step, across in enumerate(SIDES[begin:end]):
        from_x = (x - jnp.where(core == 0, side, across) + n_x) % n_x
        from_y = (y - jnp.where(core == 0, across, side) + n_y) % n_y
        for j in range(n_z):
            z = j % (n_z // 2) + core * (n_z // 2)
            owner = core if j < n_z // 2 else 1 - core
            base = ((z * 2 + from_x // 2) * 2 + owner) * 2 * n_y + from_y * 2 + from_x % 2
            at = (step * n_z + j) * piece
            id_ref[at : at + piece, :] = row + base * piece
    dt_ref[...] = d_ref[...].T

    def front(tile, slot):
        cols = pl.ds(pl.multiple_of(tile * QT, QT), QT)
        q_t = qt_ref[:, cols]
        off = off_ref[:, cols]
        w = w_ref[:, cols]
        pos = pos_ref[:, cols]
        found = jnp.zeros((8, QT), F32)
        for r in range(0, nd, SUB):
            scores = jnp.dot(d_ref[r : r + SUB, :], q_t, preferred_element_type=F32)
            probs = jnp.exp2(scores * (0.0625 * LOG2E) - off)
            hits = jnp.concatenate([id_ref[r : r + SUB, :]] * (QT // 128), 1) == pos
            c_ref[slot, r : r + SUB, :] = (probs - jnp.where(hits, w, 0.0)).astype(BF16)
            found = found + jnp.sum(jnp.where(hits, scores, 0.0).reshape(SUB // 8, 8, QT), 0)
        if not first:
            found = found_in[:, cols] + found
        if last:
            found = 0.0625 * w * found
            width = found_ref.shape[1]
            for c in range(0, QT, width):
                found_ref[...] -= found[:, c : c + width]
        else:
            found_ref[:, cols] = found

    def back(tile, slot, opening=False, closing=False):
        cols = pl.ds(pl.multiple_of(tile * QT, QT), QT)
        q = q_ref[cols, :]
        leave = []
        for r in range(0, nd, SUB):
            rows = slice(r, r + SUB)
            term = jnp.dot(c_ref[slot, rows, :], q, preferred_element_type=F32)
            if not opening:
                term = gd_ref[rows, :] + term
            if closing and kept:
                gd_refs[r // split][r % split : r % split + SUB, :] = term
            else:
                gd_ref[rows, :] = term
            if closing and not kept:
                out = gd_refs[r // split].at[pl.ds(r % split, SUB)]
                leave.append(pltpu.make_async_copy(gd_ref.at[rows], out, sems.at[r // SUB]))
                leave[-1].start()
        term = jnp.dot(dt_ref[...], c_ref[slot], preferred_element_type=F32)
        gq_ref[:, cols] = term if first else gq_in[:, cols] + term
        if closing and last:
            gd_refs[-1][split:, :] = found_ref[...]
        for copy in leave:
            copy.wait()

    tiles = nq // QT
    front(0, 0)
    front(1, 1)
    back(0, 0, opening=True)

    def pair(i, _):
        tile = 2 * i + 1
        front(tile + 1, 0)
        back(tile, 1)
        front(tile + 2, 1)
        back(tile + 1, 0)
        return 0

    lax.fori_loop(0, (tiles - 2) // 2, pair, 0)
    back(tiles - 1, 1, closing=True)


def fused(turn, split, place, docs, asked, ends, sums, sizes):
    first, last = turn == 0, turn == len(TURNS) - 1
    nq = asked[0].shape[0] * (2 if first else 1)
    width = docs.shape[1]
    _, begin, end = TURNS[turn]
    nd = docs.shape[0] // len(SIDES) * (end - begin)
    vmem = pl.BlockSpec(memory_space=pltpu.VMEM)
    hbm = pl.BlockSpec(memory_space=pltpu.HBM)
    operands = [place, docs, *asked, ends, *sums]
    outs = nd // split
    kept = turn >= KEPT
    sums_shape = (split + 8 if last else split, width)
    out_shape = [jax.ShapeDtypeStruct(sums_shape, F32) if kept else pltpu.HBM(sums_shape, F32)] * outs
    out_shape += [jax.ShapeDtypeStruct((width, nq), F32), jax.ShapeDtypeStruct((8, width if last else nq), F32)]
    if first:
        line = jax.ShapeDtypeStruct((1, nq), F32)
        out_shape += [jax.ShapeDtypeStruct((nq, width), BF16), jax.ShapeDtypeStruct((width, nq), BF16)]
        out_shape += [line, line, jax.ShapeDtypeStruct((1, nq), jnp.int32)]
    return pl.pallas_call(
        functools.partial(kernel, sizes, turn, split),
        in_specs=[pl.BlockSpec(memory_space=pltpu.SMEM), vmem, hbm if first else vmem] + [vmem] * (len(operands) - 3),
        out_specs=[vmem if kept else hbm] * outs + [vmem] * (len(out_shape) - outs),
        out_shape=out_shape,
        scratch_shapes=[
            pltpu.VMEM((width, nd), BF16),
            pltpu.VMEM((nd, 128), jnp.int32),
            pltpu.VMEM((2, nd, QT), BF16),
            pltpu.VMEM((nd, width), F32),
            pltpu.SemaphoreType.DMA((nd // SUB + 1,)),
        ],
        input_output_aliases={} if first else {8: outs},
        compiler_params=pltpu.CompilerParams(vmem_limit_bytes=VMEM_LIMIT),
        cost_estimate=pl.CostEstimate(flops=6 * nq * nd * width, bytes_accessed=8 << 20, transcendentals=nq * nd),
        name="fused",
    )(*operands)


def all_sides(array, along):
    sides = {}
    for side in (0, 2, 1, -1):
        sides[side] = moved(array, along, side)
    return sides


def on_device(queries, documents, log_norms, weights, positives):
    own, width = queries.shape
    piece = documents.shape[0]
    total_q = own * lax.axis_size(AXES)
    n_x, n_y, n_z = lax.axis_size(X), lax.axis_size(Y), lax.axis_size("z")
    place = jnp.stack([lax.axis_index(X), lax.axis_index(Y), lax.axis_index("core")]).astype(jnp.int32)
    core = lax.axis_index("core")

    rows = jnp.stack([log_norms, weights, positives.astype(F32)])
    others = other_core(queries), other_core(rows)
    asked = (pltpu.with_memory_space_constraint(queries, pltpu.HBM), others[0], rows, others[1])

    column = lax.all_to_all(jnp.broadcast_to(documents[None], (n_z, piece, width)), "z", 0, 0, tiled=True)
    low, high = column.reshape(2, n_z // 2 * piece, width)
    mine, others = jnp.where(core == 0, low, high), jnp.where(core == 0, high, low)
    part = jnp.concatenate([mine, other_core(others)])
    near = all_sides(part, False)
    docs = all_sides(jnp.concatenate([near[s] for s in SIDES]), True)

    nd = docs[0].shape[0]
    terms = {}
    ends = (weights * log_norms).reshape(-1, width).sum(0)[None]
    sums = ()
    for turn, (side, begin, end) in enumerate(TURNS):
        count = nd // len(SIDES) * (end - begin)
        outs = 2 if side == 2 else 1
        got = fused(turn, count // outs, place, docs[side], asked, ends, sums, (n_x, n_y, n_z))
        terms.setdefault(side, []).extend(got[:outs])
        sums = grad_q, lost = got[outs : outs + 2]
        asked = got[outs + 2 :] or asked

    n = nd // 2
    far_a = moved(terms[2][0], True, -1)
    far_b = moved(terms[2][1], True, 1)
    behind = moved(jnp.concatenate([terms[-1][0][:n], terms[-1][0][n:] + far_b]), True, 1)
    ahead_a = moved(terms[1][0] + far_a, True, -1)
    ahead_b = moved(terms[1][1], True, -1)
    lost = lost + moved(lost, True, 1) + moved(lost, True, 2) + ahead_b[n:]
    total = terms[0][0] + jnp.concatenate([ahead_a, ahead_b[:n]]) + behind
    n = nd // 4
    part = jnp.concatenate([total[:n], lost])
    for i, side in enumerate(SIDES):
        if side:
            part = part + moved(jnp.concatenate([total[i * n : (i + 1) * n], lost]), False, -side)
    mine, given = part[: n // 2], part[n // 2 :]
    got = other_core(given)
    lost = given[n // 2 :] + got[n // 2 :]
    got = got[: n // 2]
    low, high = jnp.where(core == 0, mine, got), jnp.where(core == 0, got, mine)
    fold = width // 2
    part = jnp.concatenate([low, high])
    sides = [part[:, i : i + fold].reshape(n_z, piece, fold) for i in (0, fold)]
    lost = lost[:, :fold] + lost[:, fold:]
    part = jnp.concatenate([*sides, jnp.broadcast_to(lost[None], (n_z, 8, fold))], 1)
    part = lax.all_to_all(part, "z", 0, 0, tiled=True)
    loss = jnp.sum(part[:, 2 * piece :]) / total_q
    part = part[:, : 2 * piece].sum(0)
    part = jnp.concatenate([part[:piece], part[piece:]], 1)
    grad_documents = (part * 0.0625).astype(BF16)

    other_grad = grad_q[:, own:]
    other_grad = other_core(other_grad)
    grad_queries = ((grad_q[:, :own] + other_grad).T * 0.0625).astype(BF16)
    return (grad_queries, grad_documents, loss)


def solution(mesh):
    torus = Mesh(mesh.devices.reshape(8, 2, 2, 4, 2), AXES)
    placed = (P(AXES, None), P(AXES, None), P(AXES), P(AXES), P(AXES))
    return jax.shard_map(
        on_device,
        mesh=torus,
        in_specs=placed,
        out_specs=(P(AXES, None), P(AXES, None), P()),
        check_vma=False,
    )
```
